32 devices in a mesh: sub: 16 (over z, y, core), tm: 2 (over x).
Axes of the slice: x: 2, y: 2, z: 4, core: 2. Of those that a mesh axis runs over, the one named last changes fastest.
Arguments:
- voltages: bfloat16 [192, 2, 96, 2048], P('sub', None, None, 'tm'), may hold values from -6 to 6
- pointing_table: bfloat16 [192, 2, 320, 96], P('sub'), may hold values from -0.4375 to 0.4375
- beam_pointing: int32 [256], replicated, may hold values from 0 to 319
- subband_order: int32 [192], replicated, may hold values from 0 to 191, each once
- live_subbands: int32 [1], replicated, may hold values from 152 to 192
- filter_taps: float32 [16, 16], replicated, may hold values from -0.36 to 0.36
Outputs:
- synthesised: bfloat16 [256, 12, 2, 32768], P('sub', None, None, 'tm')
The draws below stay inside these ranges and needn't reach their ends.
Inputs may be any that keep to these rules, and one draw needn't show every extreme that they name: `subband_order`: each slot is named by exactly one frequency.
All inputs are finite; a program needn't handle non-finite values.
Results may differ from the reference program's by a relative error of at most 0.0052.
Values may be sent and summed in bfloat16 or wider, within the bound.
A program may use at most 192 MiB of HBM per device.

```python
import math
import jax
import jax.numpy as jnp
from jax import lax

INPUTS = 96
BEAMS = 256
POINTINGS = 320
CHAN = 16
TAPS = 16
SUBBANDS = 192
TIME = 2048


def draw_live_subbands(key, part):
    span = 2 * CHAN + CHAN // 2
    raw = jax.random.randint(jax.random.fold_in(key, 7919), (1,), -span, span + 1, dtype=jnp.int32)
    missing = jnp.maximum(raw, 0)
    return (SUBBANDS - missing).astype(jnp.int32)


def place_ends(drawn, rng, smallest, top_value):
    longest = drawn.shape.index(max(drawn.shape))
    spots = []
    for shift in (0, 1):
        where = [jax.random.randint(jax.random.fold_in(rng, axis), (), 0, length) for axis, length in enumerate(drawn.shape)]
        where[longest] = (where[longest] + shift) % drawn.shape[longest]
        spots.append(tuple(where))
    return drawn.at[spots[0]].set(smallest).at[spots[1]].set(top_value)


def levels(key, shape, cuts, least, top_value):
    def one(axis_at, blocks):
        steps = jax.random.uniform(jax.random.fold_in(jax.random.fold_in(key, 6), axis_at), (blocks,), jnp.float32, least / len(cuts), top_value / len(cuts))
        return jnp.repeat(jnp.exp(steps), shape[axis_at] // blocks).reshape((-1,) + (1,) * (len(shape) - axis_at - 1))

    loudness = one(*cuts[0])
    for cut in cuts[1:]:
        loudness = loudness * one(*cut)
    return loudness


def gaussian(own_key, dims, spread, bound, pieces=(), held_as=jnp.bfloat16):
    array = spread * jax.random.normal(own_key, dims, jnp.float32)
    if pieces:
        array = array * levels(own_key, dims, pieces, -0.22, 0.18)
    return jnp.clip(array, -bound, bound).astype(held_as)


def setup_inputs(seed: int = 0) -> dict:
    key_of = jax.random.split(jax.random.key(seed), 7)
    return {
        "voltages": gaussian(key_of[0], (SUBBANDS, 2, INPUTS, TIME), 1.0, 6.0, ((0, 16), (3, 2))),
        "pointing_table": gaussian(key_of[1], (SUBBANDS, 2, POINTINGS, INPUTS), (2 * INPUTS) ** -0.5, 0.4375, ((0, 16),)),
        "beam_pointing": place_ends(jax.random.randint(key_of[2], (BEAMS,), 0, POINTINGS), jax.random.fold_in(key_of[2], 1), 0, POINTINGS - 1).astype(jnp.int32),
        "subband_order": jax.random.permutation(key_of[3], SUBBANDS).astype(jnp.int32),
        "live_subbands": draw_live_subbands(jax.random.fold_in(key_of[6], 71), 0),
        "filter_taps": gaussian(key_of[5], (TAPS, CHAN), 0.06, 0.36, (), jnp.float32),
    }


def inverse_table(channel_count):
    channel_index = jnp.arange(channel_count, dtype=jnp.int32)
    phase = (jnp.outer(channel_index, channel_index) % channel_count).astype(jnp.float32) * (2.0 * math.pi / channel_count)
    cosine = jnp.cos(phase).astype(jnp.bfloat16)
    sine_table = jnp.sin(phase).astype(jnp.bfloat16)
    upper_rows = jnp.stack([cosine, -sine_table], axis=1)
    lower_rows = jnp.stack([sine_table, cosine], axis=1)
    return jnp.stack([upper_rows, lower_rows], axis=0)


def reference(voltages, pointing_table, beam_pointing, subband_order, live_subbands, filter_taps):
    highest = lax.Precision.HIGHEST

    def form_subband(subband_pair):
        table_rows, signal = subband_pair
        chosen = jnp.take(table_rows, beam_pointing, axis=1).astype(jnp.float32)
        signal = signal.astype(jnp.float32)
        real_part = jnp.dot(chosen[0], signal[0], precision=highest) - jnp.dot(chosen[1], signal[1], precision=highest)
        imag_part = jnp.dot(chosen[1], signal[0], precision=highest) + jnp.dot(chosen[0], signal[1], precision=highest)
        return jnp.stack([real_part, imag_part], axis=1).astype(jnp.bfloat16)

    formed = lax.map(form_subband, (pointing_table, voltages))
    inverse_rows = inverse_table(CHAN).astype(jnp.float32)
    live_mask = jnp.arange(SUBBANDS, dtype=jnp.int32) < live_subbands[0]
    length = formed.shape[3]

    def synth_beam(beam_index):
        beam_rows = lax.dynamic_index_in_dim(formed, beam_index, 1, keepdims=False)
        spectrum = jnp.take(beam_rows, subband_order, axis=0)
        spectrum = jnp.where(live_mask[:, None, None], spectrum, jnp.zeros_like(spectrum))
        grouped = spectrum.astype(jnp.float32).reshape(SUBBANDS // CHAN, CHAN, 2, length)
        channels = jnp.einsum('qkpc,gcpt->gqkt', inverse_rows, grouped, precision=highest)
        extended = jnp.pad(channels, ((0, 0), (0, 0), (0, 0), (TAPS - 1, 0)))
        running = jnp.zeros_like(channels)
        for tap_index in range(TAPS):
            offset = TAPS - 1 - tap_index
            running = running + filter_taps[tap_index][:, None] * extended[..., offset:offset + length]
        return jnp.swapaxes(running, 2, 3).reshape(SUBBANDS // CHAN, 2, length * CHAN).astype(jnp.bfloat16)

    return lax.map(synth_beam, jnp.arange(BEAMS, dtype=jnp.int32))
```

```python
import functools
import math

import jax
import jax.numpy as jnp
from jax import lax
from jax.experimental import pallas as pl
from jax.experimental.pallas import tpu as pltpu
from jax.sharding import PartitionSpec as P

LANES = 128
VMEM = 60 * 1024 * 1024


def inverse_table(channel_count):
    channel_index = jnp.arange(channel_count, dtype=jnp.int32)
    phase = (jnp.outer(channel_index, channel_index) % channel_count).astype(jnp.float32) * (
        2.0 * math.pi / channel_count
    )
    cosine = jnp.cos(phase).astype(jnp.bfloat16)
    sine_table = jnp.sin(phase).astype(jnp.bfloat16)
    upper_rows = jnp.stack([cosine, -sine_table], axis=1)
    lower_rows = jnp.stack([sine_table, cosine], axis=1)
    return jnp.stack([upper_rows, lower_rows], axis=0)


def synthesis_matrix(filter_taps, inner, reach):
    tap_count, chan = filter_taps.shape
    table = inverse_table(chan).astype(jnp.float32)
    delta = jnp.arange(reach)[:, None, None]
    tl_in = jnp.arange(inner)[None, :, None]
    tl_out = jnp.arange(inner)[None, None, :]
    tap = inner * delta + tl_out - tl_in
    inside = (tap >= 0) & (tap < tap_count)
    taps = jnp.where(inside[..., None], filter_taps[jnp.clip(tap, 0, tap_count - 1)], 0.0)
    full = (
        taps[:, None, :, None, None, :, :]
        * table.transpose(2, 3, 0, 1)[None, :, None, :, :, None, :]
    )
    return full.reshape(reach * 2 * inner * chan, 2 * inner * chan).astype(jnp.bfloat16)


def form_kernel(inner, groups, with_rim, hot_ref, perm_ref, table_ref, volt_ref, *rest):
    chunks = rest[-len(groups) :]
    f32, bf16 = jnp.float32, jnp.bfloat16
    real, imag = table_ref[0, 0], table_ref[0, 1]
    both = jnp.concatenate(
        [
            jnp.concatenate([real, -imag], axis=1),
            jnp.concatenate([imag, real], axis=1),
        ],
        axis=0,
    )
    weights = jnp.dot(hot_ref[...], both, preferred_element_type=f32).astype(bf16)
    if with_rim:
        rim_ref, rim_out = rest[0], rest[1]
        rim_out[0] = jnp.dot(weights, rim_ref[0], preferred_element_type=f32).astype(bf16)
    signal = jnp.dot(volt_ref[0], perm_ref[...], preferred_element_type=f32).astype(bf16)
    start = 0 if with_rim else hot_ref.shape[0] - 2 * sum(groups) * chunks[0].shape[0]
    for group, out in zip(groups, chunks):
        rows = 2 * group * out.shape[0]
        formed = jnp.dot(
            weights[start : start + rows], signal, preferred_element_type=f32
        ).astype(bf16)
        start += rows
        for d in range(out.shape[0]):
            for tl in range(inner):
                out[d, 0, tl] = formed[
                    2 * d * group : 2 * (d + 1) * group, tl * LANES : (tl + 1) * LANES
                ]


def synth_kernel(
    inner, chan, group, reach, local, order_ref, live_ref, z_ref, rim_ref, mat_ref, *rest
):
    out_ref, held, wide, line, stacked, made, sems = rest[-7:]
    g = pl.program_id(0)
    count = pl.num_programs(0)
    f32, bf16 = jnp.float32, jnp.bfloat16

    def fetch(step, slot):
        named = [order_ref[step * chan + c] for c in range(chan)]
        return [
            pltpu.make_async_copy(
                z_ref.at[lax.div(at, local), pl.ds(lax.rem(at, local) * inner, inner)],
                held.at[slot, c],
                sems.at[slot],
            )
            for c, at in enumerate(named)
        ]

    slot = lax.rem(g, 2)

    @pl.when(g == 0)
    def _():
        for copy in fetch(0, 0):
            copy.start()

    @pl.when(g + 1 < count)
    def _():
        for copy in fetch(g + 1, 1 - slot):
            copy.start()

    for copy in fetch(g, slot):
        copy.wait()

    pair = 2 * group
    for c in range(chan):
        alive = g * chan + c < live_ref[0]
        for tl in range(inner):
            block = held[slot, c, tl].astype(f32)
            wide[tl, c * pair : (c + 1) * pair, :] = jnp.where(alive, block, 0.0)

    width = inner * chan

    def turn(b, carry):
        base = pl.multiple_of(b * LANES, LANES)
        for p in range(2):
            rows = [
                wide[tl, pl.ds(p * group + b, chan, stride=pair), :] for tl in range(inner)
            ]
            line[p, 8 : 8 + LANES, :] = jnp.concatenate(rows, axis=0).T
            line[p, 8 - (reach - 1) : 8, :] = rim_ref[0, b, p]
            for delta in range(reach):
                at = (2 * delta + p) * width
                stacked[pl.ds(base, LANES), at : at + width] = line[
                    p, 8 - delta : 8 - delta + LANES, :
                ].astype(bf16)
        return carry

    lax.fori_loop(0, group, turn, 0, unroll=2)

    def emit(b, carry):
        base = pl.multiple_of(b * 2 * LANES, 2 * LANES)
        out = jnp.dot(
            stacked[pl.ds(base, 2 * LANES), :], mat_ref[...], preferred_element_type=f32
        )
        for i in range(2):
            for q in range(2):
                made[i, q * LANES : (q + 1) * LANES, :] = out[
                    i * LANES : (i + 1) * LANES, q * width : (q + 1) * width
                ]
        for i in range(2):
            for tb in range(LANES):
                both = made[i, pl.ds(tb, 2, stride=LANES), :].astype(bf16)
                out_ref[2 * b + i, 0, :, tb * LANES : (tb + 1) * LANES] = both
        return carry

    lax.fori_loop(0, group // 2, emit, 0)


def direct_plan(voltages, pointing_table, beam_pointing, subband_order, live_subbands, filter_taps):
    local_subbands, _, inputs, local_time = voltages.shape
    pointings = pointing_table.shape[2]
    beam_count = beam_pointing.shape[0]
    slots = subband_order.shape[0]
    tap_count, chan = filter_taps.shape
    inner = LANES // chan
    assert local_time == inner * LANES
    reach = 1 + -(-(tap_count - 1) // inner)
    rim_len = (reach - 1) * inner
    devices = lax.axis_size("sub")
    beam_part = beam_count // devices
    quarter = beam_part // 4
    if beam_part % 8 == 0:
        groups, firsts = [quarter, 2 * quarter, quarter], [0, 2 * quarter, quarter]
    else:
        groups, firsts = [beam_part], [0]
    starts = [sum(groups[:h]) for h in range(len(groups))]
    bands = slots // chan

    signal = voltages.reshape(local_subbands, 2 * inputs, local_time)
    times = range(lax.axis_size("tm"))
    route = [(i - 1, i) for i in times if i > 0]
    rim = lax.ppermute(signal[:, :, local_time - rim_len :], "tm", route)
    rim = jnp.pad(rim, ((0, 0), (0, 0), (0, LANES - rim_len)))

    picks = beam_pointing.reshape(devices, beam_part)
    wanted = jnp.concatenate(
        [
            (
                picks[:, None, first : first + group]
                + pointings * jnp.arange(2, dtype=jnp.int32)[:, None]
            ).reshape(-1)
            for first, group in zip(firsts, groups)
        ]
    )
    hot = (wanted[:, None] == jnp.arange(2 * pointings)[None, :]).astype(jnp.bfloat16)
    source = jnp.arange(local_time, dtype=jnp.int32)
    place = (source % inner) * LANES + source // inner
    perm = (place[:, None] == source[None, :]).astype(jnp.bfloat16)

    def form(groups, signal, rim):
        with_rim = rim is not None
        pieces = [(devices, local_subbands, inner, 2 * group, LANES) for group in groups]
        rim_size = (local_subbands, hot.shape[0], LANES)
        return pl.pallas_call(
            functools.partial(form_kernel, inner, groups, with_rim),
            grid=(local_subbands,),
            in_specs=[
                pl.BlockSpec(hot.shape, lambda s: (0, 0)),
                pl.BlockSpec(perm.shape, lambda s: (0, 0)),
                pl.BlockSpec((1, 2, pointings, inputs), lambda s: (s, 0, 0, 0)),
                pl.BlockSpec((1, 2 * inputs, local_time), lambda s: (s, 0, 0)),
            ]
            + [pl.BlockSpec((1, 2 * inputs, LANES), lambda s: (s, 0, 0))] * with_rim,
            out_specs=[pl.BlockSpec((1,) + rim_size[1:], lambda s: (s, 0, 0))] * with_rim
            + [
                pl.BlockSpec((size[0], 1) + size[2:], lambda s: (0, s, 0, 0, 0))
                for size in pieces
            ],
            out_shape=[jax.ShapeDtypeStruct(rim_size, jnp.bfloat16)] * with_rim
            + [jax.ShapeDtypeStruct(size, jnp.bfloat16) for size in pieces],
            compiler_params=pltpu.CompilerParams(vmem_limit_bytes=VMEM),
            cost_estimate=pl.CostEstimate(
                flops=12_000_000_000, bytes_accessed=20_000_000, transcendentals=0
            ),
            name="form",
        )(hot, perm, pointing_table, signal, *([rim] if with_rim else []))

    edge, opening = form(groups[:1], signal, rim)
    pieces = [opening]
    if len(groups) > 1:
        later, _ = lax.optimization_barrier((signal, opening))
        pieces += form(groups[1:], later, None)

    mat = synthesis_matrix(filter_taps, inner, reach)

    edge = edge[:, :, :rim_len]
    edge = jnp.concatenate(
        [
            edge[:, 2 * devices * start : 2 * devices * (start + group)].reshape(
                local_subbands, devices, 2 * group * rim_len
            )
            for start, group in zip(starts, groups)
        ],
        axis=2,
    )
    edge = edge.swapaxes(0, 1).reshape(devices, -1)
    edge_size = edge.shape[1]
    planes = -(-edge_size // (2 * groups[0] * LANES))
    edge = jnp.pad(edge, ((0, 0), (0, planes * 2 * groups[0] * LANES - edge_size)))
    edge = edge.reshape(devices, planes, 2 * groups[0], LANES)
    pieces = [
        piece.reshape(devices, local_subbands * inner, 2 * group, LANES)
        for piece, group in zip(pieces, groups)
    ]
    pieces[0] = jnp.concatenate([pieces[0], edge], axis=1)
    got = [lax.all_to_all(p, "sub", split_axis=0, concat_axis=0, tiled=True) for p in pieces]
    edge = got[0][:, local_subbands * inner :].reshape(devices, -1)[:, :edge_size]
    edge = jnp.take(edge.reshape(slots, -1), subband_order, axis=0)
    live_mask = jnp.arange(slots, dtype=jnp.int32) < live_subbands[0]
    edge = jnp.where(live_mask[:, None], edge.astype(jnp.float32), 0.0)

    def edge_of(start, group):
        part = edge[:, 2 * start * rim_len : 2 * (start + group) * rim_len]
        part = part.reshape(bands, chan, 2, group, reach - 1, inner)
        return part.transpose(0, 3, 2, 4, 5, 1).reshape(
            bands, group, 2, reach - 1, inner * chan
        )

    result = None
    for first, start, group, z in zip(firsts, starts, groups, got):
        operands = [subband_order, live_subbands, z, edge_of(start, group), mat]
        in_specs = [
            pl.BlockSpec(memory_space=pl.ANY),
            pl.BlockSpec((1, group, 2, reach - 1, LANES), lambda g, *_: (g, 0, 0, 0, 0)),
            pl.BlockSpec(mat.shape, lambda g, *_: (0, 0)),
        ]
        alias = {}
        if result is not None:
            operands.append(result)
            in_specs.append(pl.BlockSpec(memory_space=pl.ANY))
            alias = {5: 0}
        result = pl.pallas_call(
            functools.partial(synth_kernel, inner, chan, group, reach, local_subbands),
            grid_spec=pltpu.PrefetchScalarGridSpec(
                num_scalar_prefetch=2,
                grid=(bands,),
                in_specs=in_specs,
                out_specs=pl.BlockSpec(
                    (group, 1, 2, local_time * chan), functools.partial(lambda h, g, *_: (h, g, 0, 0), first // group)
                ),
                scratch_shapes=[
                    pltpu.VMEM((2, chan, inner, 2 * group, LANES), jnp.bfloat16),
                    pltpu.VMEM((inner, chan * 2 * group, LANES), jnp.float32),
                    pltpu.VMEM((2, 8 + LANES, LANES), jnp.float32),
                    pltpu.VMEM((group * LANES, mat.shape[0]), jnp.bfloat16),
                    pltpu.VMEM((2, 2 * LANES, LANES), jnp.float32),
                    pltpu.SemaphoreType.DMA((2,)),
                ],
            ),
            out_shape=jax.ShapeDtypeStruct((beam_part, bands, 2, local_time * chan), jnp.bfloat16),
            input_output_aliases=alias,
            compiler_params=pltpu.CompilerParams(vmem_limit_bytes=VMEM),
            cost_estimate=pl.CostEstimate(
                flops=10_000_000_000, bytes_accessed=13_000_000, transcendentals=0
            ),
            name="synth",
        )(*operands)

    return result

MESH = pl.DeviceIdType.MESH


def drain(ref, sem):
    pltpu.make_async_copy(ref, ref, sem).wait()


def relay_kernel(
    n,
    chan,
    order_ref,
    live_ref,
    pick_ref,
    table_ref,
    taps_ref,
    trig_ref,
    volt_ref,
    out_ref,
    z,
    own_out,
    far_out,
    volts,
    far_volts,
    chosen,
    far_chosen,
    own_w,
    far_w,
    lhs,
    stage,
    wide,
    line,
    mat,
    made,
    ready,
    tail,
    tail_sent,
    rim,
    z_sem,
    own_sem,
    far_sem,
    in_sem,
    volt_send,
    volt_recv,
    w_send,
    w_recv,
    fwd_send,
    fwd_recv,
    rim_sem,
    out_sem,
):
    f32, bf16 = jnp.float32, jnp.bfloat16
    half, quarter = n // 2, n // 4
    chunks, slots_here, inputs2, _ = volts.shape
    pair = z.shape[2]
    group = pair // 2
    bands = ready.shape[1]
    inner = LANES // chan
    spans = mat.shape[0] // pair_of(chan)
    halo = spans - inner
    blocks = LANES // inner
    ring = far_out.shape[0]

    me, tm = lax.axis_index("sub"), lax.axis_index("tm")
    side, pos = lax.div(me, half), lax.rem(me, half)
    rank, lane = lax.div(pos, quarter), lax.rem(me, quarter)
    other = 1 - side
    is_gate = rank == 1 - side
    gate = other * half + side * quarter + lane
    share = slots_here // 2
    mine = pl.ds(tm * share, share)
    theirs = pl.ds((1 - tm) * share, share)

    def chunk_at(step):
        return lax.rem(step + chunks - 1, chunks)

    def source_of(rank_from):
        return other * half + rank_from * quarter + lane

    def load(c):
        return pltpu.make_async_copy(
            volt_ref.at[:, :, pl.ds(pl.multiple_of(c * LANES, LANES), LANES)],
            volts.at[c],
            in_sem.at[c],
        )

    def send_volts(c):
        pltpu.make_async_remote_copy(
            src_ref=volts.at[c],
            dst_ref=far_volts.at[c, rank],
            send_sem=volt_send.at[c],
            recv_sem=volt_recv.at[c, rank],
            device_id=(gate, tm),
            device_id_type=MESH,
        ).start()

    def send_all(sent, src, c, sems):
        def to(j, carry):
            there = lax.rem(pos + 1 + j, half)
            pltpu.make_async_remote_copy(
                src_ref=sent.at[there],
                dst_ref=z.at[c, pl.ds(src * slots_here, slots_here)],
                send_sem=sems.at[there],
                recv_sem=z_sem.at[c, src],
                device_id=(side * half + there, tm),
                device_id_type=MESH,
            ).start()
            return carry

        lax.fori_loop(0, half - 1, to, 0)

    def wait_all(sent, sems):
        def one(j, carry):
            there = lax.rem(pos + 1 + j, half)
            drain(sent.at[there], sems.at[there])
            return carry

        lax.fori_loop(0, half - 1, one, 0)

    def form(weights, signal, sent, src, c):
        def one(s, carry):
            formed = jnp.dot(
                weights[s][:, :inputs2], signal[s], preferred_element_type=f32
            ).astype(bf16)
            for d in range(half):
                sent[d, s] = formed[d * pair : (d + 1) * pair]
            return carry

        lax.fori_loop(0, slots_here, one, 0)

        def keep(s, carry):
            z[c, src * slots_here + s] = sent[pos, s]
            return carry

        lax.fori_loop(0, slots_here, keep, 0)

    def prepare(picked, weights, at):
        w = picked.astype(f32)
        real, imag = w[: inputs2 // 2], w[inputs2 // 2 :]
        rest = jnp.zeros((weights.shape[2] - inputs2, LANES), f32)
        upper = jnp.concatenate([real, -imag, rest], axis=0).T.astype(bf16)
        lower = jnp.concatenate([imag, real, rest], axis=0).T.astype(bf16)
        for d in range(half):
            rows = slice(d * group, (d + 1) * group)
            weights[at, d * pair : d * pair + group] = upper[rows]
            weights[at, d * pair + group : (d + 1) * pair] = lower[rows]

    for step in range(chunks):
        load(chunk_at(step)).start()
    load(chunk_at(0)).wait()
    send_volts(chunk_at(0))

    pointings = table_ref.shape[2]
    hot = (
        lax.broadcasted_iota(jnp.int32, (pointings, 2 * LANES), 0) == pick_ref[...]
    ).astype(bf16)

    def choose(s, carry):
        picked = jnp.dot(table_ref[s], hot, preferred_element_type=f32).astype(bf16)
        chosen[0, s] = picked[:, :LANES]
        chosen[1, s] = picked[:, LANES:]
        return carry

    lax.fori_loop(0, slots_here, choose, 0)
    pltpu.make_async_remote_copy(
        src_ref=chosen.at[other, mine],
        dst_ref=far_chosen.at[rank, mine],
        send_sem=w_send,
        recv_sem=w_recv.at[rank],
        device_id=(gate, tm),
        device_id_type=MESH,
    ).start()
    load(chunk_at(1)).wait()
    send_volts(chunk_at(1))

    def prepare_own(s, carry):
        prepare(chosen[side, s], own_w, s)
        return carry

    lax.fori_loop(0, slots_here, prepare_own, 0)

    for v in range(spans):
        taps = taps_ref[v : v + 1, :]
        mat[v * 2 * chan : (v + 1) * 2 * chan] = (
            jnp.concatenate([taps, taps], axis=1) * trig_ref[...]
        ).astype(bf16)
    tail[...] = jnp.zeros_like(tail)

    def foreign_weights():
        def forward(k):
            return pltpu.make_async_remote_copy(
                src_ref=far_chosen.at[k, mine],
                dst_ref=far_chosen.at[k, mine],
                send_sem=fwd_send.at[k],
                recv_sem=fwd_recv.at[k],
                device_id=(me, 1 - tm),
                device_id_type=MESH,
            )

        for k in range(2):
            drain(far_chosen.at[k, mine], w_recv.at[k])
            forward(k).start()
        for k in range(2):
            drain(far_chosen.at[k, theirs], fwd_recv.at[k])
        for k in range(2):

            def one(s, carry):
                prepare(far_chosen[k, s], far_w.at[k], s)
                return carry

            lax.fori_loop(0, slots_here, one, 0)
        for k in range(2):
            drain(far_chosen.at[k, mine], fwd_send.at[k])

    lanes_at = lax.broadcasted_iota(jnp.int32, (blocks, LANES), 1)
    width = 2 * chan
    fold = LANES // width

    def synthesise(i):
        c = chunk_at(lax.rem(i - 1, chunks))

        @pl.when(i <= chunks)
        def _():
            def one(src, carry):
                local = (src == me) | (
                    is_gate & (lax.div(src, half) == other) & (lax.rem(src, quarter) == lane)
                )

                @pl.when(jnp.logical_not(local))
                def _():
                    drain(z.at[c, pl.ds(src * slots_here, slots_here)], z_sem.at[c, src])

                return carry

            lax.fori_loop(0, n, one, 0)

        def copy(s, carry):
            stage[s] = z[c, s]
            return carry

        lax.fori_loop(0, stage.shape[0], copy, 0, unroll=4)

        def gather(g, carry):
            for k in range(chan):
                alive = g * chan + k < live_ref[0]
                block = stage[order_ref[g * chan + k]].astype(f32)
                wide[k * pair : (k + 1) * pair] = jnp.where(alive, block, 0.0)

            def turn(q, carry):
                rows = [
                    wide[pl.ds(p * group + q * fold + b, chan, stride=pair), :]
                    for b in range(fold)
                    for p in range(2)
                ]
                turned = jnp.concatenate(rows, axis=0).T
                at = g * (group // fold) + q
                line[:halo] = tail[at]
                line[halo : halo + LANES] = turned
                tail[at] = turned[LANES - halo :]
                for u in range(spans // fold):
                    parts = [
                        line[pl.ds(u * fold + w, blocks, stride=inner), :] for w in range(fold)
                    ]
                    for b in range(fold):
                        block = None
                        for w in range(fold):
                            shift = (w - b) * width % LANES
                            part = pltpu.roll(parts[w], shift, 1) if shift else parts[w]
                            if block is None:
                                block = part
                            else:
                                block = jnp.where(lanes_at >= w * width, part, block)
                        lhs[
                            q * fold + b,
                            pl.ds(pl.multiple_of(g * blocks, blocks), blocks),
                            u * LANES : (u + 1) * LANES,
                        ] = block.astype(bf16)
                return carry

            lax.fori_loop(0, group // fold, turn, 0)
            return carry

        lax.fori_loop(0, bands, gather, 0)

        out_copy = pltpu.make_async_copy(
            ready,
            out_ref.at[:, :, pl.ds(pl.multiple_of(c * 2 * blocks, 2 * blocks), 2 * blocks)],
            out_sem,
        )

        @pl.when(i > 1)
        def _():
            drain(ready, out_sem)

        def emit(b, carry):
            out = jnp.dot(lhs[b], mat[...], preferred_element_type=f32)
            rows = bands * blocks
            made[pl.ds(0, rows, stride=2), :] = out[:, :LANES]
            made[pl.ds(1, rows, stride=2), :] = out[:, LANES:]
            for g in range(bands):
                ready[b, g] = made[g * 2 * blocks : (g + 1) * 2 * blocks].astype(bf16)
            return carry

        lax.fori_loop(0, group, emit, 0)
        out_copy.start()

    def pass_tail():
        return pltpu.make_async_remote_copy(
            src_ref=tail_sent,
            dst_ref=rim,
            send_sem=rim_sem.at[0],
            recv_sem=rim_sem.at[1],
            device_id=(me, 1),
            device_id_type=MESH,
        )

    def step(i, carry):
        c = chunk_at(i)

        @pl.when(i + 2 < chunks)
        def _():
            later = chunk_at(i + 2)
            load(later).wait()
            send_volts(later)

        @pl.when(i < chunks)
        def _():
            form(own_w, volts.at[c], own_out.at[c], me, c)
            send_all(own_out.at[c], me, c, own_sem.at[c])

        @pl.when(is_gate & (i == 0))
        def _():
            foreign_weights()

        @pl.when(is_gate & (i < chunks))
        def _():
            turn = lax.rem(i, ring)

            def one(k, carry):
                @pl.when(i >= ring)
                def _():
                    wait_all(far_out.at[turn, k], far_sem.at[turn, k])

                drain(far_volts.at[c, k], volt_recv.at[c, k])
                src = source_of(k)
                form(far_w.at[k], far_volts.at[c, k], far_out.at[turn, k], src, c)
                send_all(far_out.at[turn, k], src, c, far_sem.at[turn, k])
                return carry

            lax.fori_loop(0, 2, one, 0)

        @pl.when((i == 2) & (tm == 0))
        def _():
            tail[...] = jnp.zeros_like(tail)

        @pl.when((i == 2) & (tm == 1))
        def _():
            drain(rim, rim_sem.at[1])
            tail[...] = rim[...]

        @pl.when(i >= 1)
        def _():
            synthesise(i)

        @pl.when((i == 1) & (tm == 0))
        def _():
            tail_sent[...] = tail[...]
            pass_tail().start()

        return carry

    lax.fori_loop(0, chunks + 2, step, 0)

    drain(ready, out_sem)
    drain(chosen.at[other, mine], w_send)

    @pl.when(tm == 0)
    def _():
        drain(tail_sent, rim_sem.at[0])

    def finish(c, carry):
        drain(volts.at[c], volt_send.at[c])
        wait_all(own_out.at[c], own_sem.at[c])
        return carry

    lax.fori_loop(0, chunks, finish, 0)

    @pl.when(is_gate)
    def _():
        def one(turn, carry):
            for k in range(2):
                wait_all(far_out.at[turn, k], far_sem.at[turn, k])
            return carry

        lax.fori_loop(0, ring, one, 0)


def pair_of(chan):
    return 2 * chan


def relay_plan(voltages, pointing_table, beam_pointing, subband_order, live_subbands, filter_taps):
    local, _, inputs, local_time = voltages.shape
    pointings = pointing_table.shape[2]
    beams = beam_pointing.shape[0]
    slots = subband_order.shape[0]
    tap_count, chan = filter_taps.shape
    n = lax.axis_size("sub")
    half = n // 2
    group = beams // n
    pair = 2 * group
    inner = LANES // chan
    spans = inner * (1 + -(-(tap_count - 1) // inner))
    halo = spans - inner
    chunks = local_time // LANES
    bands = slots // chan
    blocks = LANES // inner
    fold = LANES // (2 * chan)
    bf16, f32 = jnp.bfloat16, jnp.float32
    ring = 2

    flat = filter_taps.reshape(-1)
    before, after = (inner - 1) * chan, halo * chan + LANES - flat.shape[0]
    flat = jnp.pad(flat, (before, after))
    taps = jnp.stack(
        [
            flat[before + chan * (halo - v) : before + chan * (halo - v) + LANES]
            for v in range(spans)
        ]
    )
    trig = inverse_table(chan).astype(f32).transpose(2, 3, 0, 1)
    trig = jnp.broadcast_to(trig[:, :, :, None, :], (2, chan, 2, inner, chan))
    trig = trig.reshape(2 * chan, 2 * LANES)
    signal = voltages.reshape(local, 2 * inputs, local_time)
    table = pointing_table.transpose(0, 1, 3, 2).reshape(local, 2 * inputs, pointings)
    lanes_in = 2 * LANES

    vmem = pl.BlockSpec(memory_space=pltpu.VMEM)
    smem = pl.BlockSpec(memory_space=pltpu.SMEM)
    anywhere = pl.BlockSpec(memory_space=pl.ANY)
    dma = pltpu.SemaphoreType.DMA
    out = pl.pallas_call(
        functools.partial(relay_kernel, n, chan),
        in_specs=[smem, smem, vmem, vmem, vmem, vmem, anywhere],
        out_specs=anywhere,
        out_shape=jax.ShapeDtypeStruct((group, bands, 2 * blocks * chunks, LANES), bf16),
        scratch_shapes=[
            pltpu.VMEM((chunks, slots, pair, LANES), bf16),
            pltpu.VMEM((chunks, half, local, pair, LANES), bf16),
            pltpu.VMEM((ring, 2, half, local, pair, LANES), bf16),
            pltpu.VMEM((chunks, local, 2 * inputs, LANES), bf16),
            pltpu.VMEM((chunks, 2, local, 2 * inputs, LANES), bf16),
            pltpu.VMEM((2, local, 2 * inputs, LANES), bf16),
            pltpu.VMEM((2, local, 2 * inputs, LANES), bf16),
            pltpu.VMEM((local, half * pair, lanes_in), bf16),
            pltpu.VMEM((2, local, half * pair, lanes_in), bf16),
            pltpu.VMEM((group, bands * blocks, spans * 2 * chan), bf16),
            pltpu.VMEM((slots, pair, LANES), bf16),
            pltpu.VMEM((chan * pair, LANES), f32),
            pltpu.VMEM((halo + LANES, LANES), f32),
            pltpu.VMEM((spans * 2 * chan, 2 * LANES), bf16),
            pltpu.VMEM((bands * blocks * 2, LANES), f32),
            pltpu.VMEM((group, bands, 2 * blocks, LANES), bf16),
            pltpu.VMEM((bands * group // fold, halo, LANES), f32),
            pltpu.VMEM((bands * group // fold, halo, LANES), f32),
            pltpu.VMEM((bands * group // fold, halo, LANES), f32),
            dma((chunks, n)),
            dma((chunks, half)),
            dma((ring, 2, half)),
            dma((chunks,)),
            dma((chunks,)),
            dma((chunks, 2)),
            dma,
            dma((2,)),
            dma((2,)),
            dma((2,)),
            dma((2,)),
            dma,
        ],
        compiler_params=pltpu.CompilerParams(
            vmem_limit_bytes=66_000_000, has_side_effects=True
        ),
        cost_estimate=pl.CostEstimate(
            flops=20_000_000_000, bytes_accessed=20_000_000, transcendentals=0
        ),
        name="relay",
    )(
        subband_order,
        live_subbands,
        beam_pointing.reshape(1, beams),
        table,
        taps,
        trig,
        signal,
    )
    out = out.reshape(group, bands, blocks * chunks, 2, LANES).transpose(0, 1, 3, 2, 4)
    return out.reshape(group, bands, 2, local_time * chan)


def on_device(voltages, pointing_table, beam_pointing, subband_order, live_subbands, filter_taps):
    local, _, inputs, local_time = voltages.shape
    beams = beam_pointing.shape[0]
    n = lax.axis_size("sub")
    fits = (
        lax.axis_size("tm") == 2
        and n % 4 == 0
        and beams == 2 * LANES
        and beams // n % 8 == 0
        and local % 2 == 0
        and local_time % LANES == 0
        and local_time >= 4 * LANES
    )
    plan = relay_plan if fits else direct_plan
    return plan(
        voltages, pointing_table, beam_pointing, subband_order, live_subbands, filter_taps
    )


def solution(mesh):
    in_specs = (P("sub", None, None, "tm"), P("sub", None, None, None), P(), P(), P(), P())
    out_specs = P("sub", None, None, "tm")
    return jax.shard_map(
        on_device, mesh=mesh, in_specs=in_specs, out_specs=out_specs, check_vma=False
    )
```

```python
import functools
import math

import jax
import jax.numpy as jnp
from jax import lax
from jax.experimental import pallas as pl
from jax.experimental.pallas import tpu as pltpu
from jax.sharding import PartitionSpec as P

LANES = 128
VMEM = 60 * 1024 * 1024


def inverse_table(channel_count):
    channel_index = jnp.arange(channel_count, dtype=jnp.int32)
    phase = (jnp.outer(channel_index, channel_index) % channel_count).astype(jnp.float32) * (
        2.0 * math.pi / channel_count
    )
    cosine = jnp.cos(phase).astype(jnp.bfloat16)
    sine_table = jnp.sin(phase).astype(jnp.bfloat16)
    upper_rows = jnp.stack([cosine, -sine_table], axis=1)
    lower_rows = jnp.stack([sine_table, cosine], axis=1)
    return jnp.stack([upper_rows, lower_rows], axis=0)


def synthesis_matrix(filter_taps, inner, reach):
    tap_count, chan = filter_taps.shape
    table = inverse_table(chan).astype(jnp.float32)
    delta = jnp.arange(reach)[:, None, None]
    tl_in = jnp.arange(inner)[None, :, None]
    tl_out = jnp.arange(inner)[None, None, :]
    tap = inner * delta + tl_out - tl_in
    inside = (tap >= 0) & (tap < tap_count)
    taps = jnp.where(inside[..., None], filter_taps[jnp.clip(tap, 0, tap_count - 1)], 0.0)
    full = (
        taps[:, None, :, None, None, :, :]
        * table.transpose(2, 3, 0, 1)[None, :, None, :, :, None, :]
    )
    return full.reshape(reach * 2 * inner * chan, 2 * inner * chan).astype(jnp.bfloat16)


def form_kernel(inner, groups, with_rim, hot_ref, perm_ref, table_ref, volt_ref, *rest):
    chunks = rest[-len(groups) :]
    f32, bf16 = jnp.float32, jnp.bfloat16
    real, imag = table_ref[0, 0], table_ref[0, 1]
    both = jnp.concatenate(
        [
            jnp.concatenate([real, -imag], axis=1),
            jnp.concatenate([imag, real], axis=1),
        ],
        axis=0,
    )
    weights = jnp.dot(hot_ref[...], both, preferred_element_type=f32).astype(bf16)
    if with_rim:
        rim_ref, rim_out = rest[0], rest[1]
        rim_out[0] = jnp.dot(weights, rim_ref[0], preferred_element_type=f32).astype(bf16)
    signal = jnp.dot(volt_ref[0], perm_ref[...], preferred_element_type=f32).astype(bf16)
    start = 0 if with_rim else hot_ref.shape[0] - 2 * sum(groups) * chunks[0].shape[0]
    for group, out in zip(groups, chunks):
        rows = 2 * group * out.shape[0]
        formed = jnp.dot(
            weights[start : start + rows], signal, preferred_element_type=f32
        ).astype(bf16)
        start += rows
        for d in range(out.shape[0]):
            for tl in range(inner):
                out[d, 0, tl] = formed[
                    2 * d * group : 2 * (d + 1) * group, tl * LANES : (tl + 1) * LANES
                ]


def synth_kernel(
    inner, chan, group, reach, local, order_ref, live_ref, z_ref, rim_ref, mat_ref, *rest
):
    out_ref, held, wide, line, stacked, made, sems = rest[-7:]
    g = pl.program_id(0)
    count = pl.num_programs(0)
    f32, bf16 = jnp.float32, jnp.bfloat16

    def fetch(step, slot):
        named = [order_ref[step * chan + c] for c in range(chan)]
        return [
            pltpu.make_async_copy(
                z_ref.at[lax.div(at, local), pl.ds(lax.rem(at, local) * inner, inner)],
                held.at[slot, c],
                sems.at[slot],
            )
            for c, at in enumerate(named)
        ]

    slot = lax.rem(g, 2)

    @pl.when(g == 0)
    def _():
        for copy in fetch(0, 0):
            copy.start()

    @pl.when(g + 1 < count)
    def _():
        for copy in fetch(g + 1, 1 - slot):
            copy.start()

    for copy in fetch(g, slot):
        copy.wait()

    pair = 2 * group
    for c in range(chan):
        alive = g * chan + c < live_ref[0]
        for tl in range(inner):
            block = held[slot, c, tl].astype(f32)
            wide[tl, c * pair : (c + 1) * pair, :] = jnp.where(alive, block, 0.0)

    width = inner * chan

    def turn(b, carry):
        base = pl.multiple_of(b * LANES, LANES)
        for p in range(2):
            rows = [
                wide[tl, pl.ds(p * group + b, chan, stride=pair), :] for tl in range(inner)
            ]
            line[p, 8 : 8 + LANES, :] = jnp.concatenate(rows, axis=0).T
            line[p, 8 - (reach - 1) : 8, :] = rim_ref[0, b, p]
            for delta in range(reach):
                at = (2 * delta + p) * width
                stacked[pl.ds(base, LANES), at : at + width] = line[
                    p, 8 - delta : 8 - delta + LANES, :
                ].astype(bf16)
        return carry

    lax.fori_loop(0, group, turn, 0, unroll=2)

    def emit(b, carry):
        base = pl.multiple_of(b * 2 * LANES, 2 * LANES)
        out = jnp.dot(
            stacked[pl.ds(base, 2 * LANES), :], mat_ref[...], preferred_element_type=f32
        )
        for i in range(2):
            for q in range(2):
                made[i, q * LANES : (q + 1) * LANES, :] = out[
                    i * LANES : (i + 1) * LANES, q * width : (q + 1) * width
                ]
        for i in range(2):
            for tb in range(LANES):
                both = made[i, pl.ds(tb, 2, stride=LANES), :].astype(bf16)
                out_ref[2 * b + i, 0, :, tb * LANES : (tb + 1) * LANES] = both
        return carry

    lax.fori_loop(0, group // 2, emit, 0)


def direct_plan(voltages, pointing_table, beam_pointing, subband_order, live_subbands, filter_taps):
    local_subbands, _, inputs, local_time = voltages.shape
    pointings = pointing_table.shape[2]
    beam_count = beam_pointing.shape[0]
    slots = subband_order.shape[0]
    tap_count, chan = filter_taps.shape
    inner = LANES // chan
    assert local_time == inner * LANES
    reach = 1 + -(-(tap_count - 1) // inner)
    rim_len = (reach - 1) * inner
    devices = lax.axis_size("sub")
    beam_part = beam_count // devices
    quarter = beam_part // 4
    if beam_part % 8 == 0:
        groups, firsts = [quarter, 2 * quarter, quarter], [0, 2 * quarter, quarter]
    else:
        groups, firsts = [beam_part], [0]
    starts = [sum(groups[:h]) for h in range(len(groups))]
    bands = slots // chan

    signal = voltages.reshape(local_subbands, 2 * inputs, local_time)
    times = range(lax.axis_size("tm"))
    route = [(i - 1, i) for i in times if i > 0]
    rim = lax.ppermute(signal[:, :, local_time - rim_len :], "tm", route)
    rim = jnp.pad(rim, ((0, 0), (0, 0), (0, LANES - rim_len)))

    picks = beam_pointing.reshape(devices, beam_part)
    wanted = jnp.concatenate(
        [
            (
                picks[:, None, first : first + group]
                + pointings * jnp.arange(2, dtype=jnp.int32)[:, None]
            ).reshape(-1)
            for first, group in zip(firsts, groups)
        ]
    )
    hot = (wanted[:, None] == jnp.arange(2 * pointings)[None, :]).astype(jnp.bfloat16)
    source = jnp.arange(local_time, dtype=jnp.int32)
    place = (source % inner) * LANES + source // inner
    perm = (place[:, None] == source[None, :]).astype(jnp.bfloat16)

    def form(groups, signal, rim):
        with_rim = rim is not None
        pieces = [(devices, local_subbands, inner, 2 * group, LANES) for group in groups]
        rim_size = (local_subbands, hot.shape[0], LANES)
        return pl.pallas_call(
            functools.partial(form_kernel, inner, groups, with_rim),
            grid=(local_subbands,),
            in_specs=[
                pl.BlockSpec(hot.shape, lambda s: (0, 0)),
                pl.BlockSpec(perm.shape, lambda s: (0, 0)),
                pl.BlockSpec((1, 2, pointings, inputs), lambda s: (s, 0, 0, 0)),
                pl.BlockSpec((1, 2 * inputs, local_time), lambda s: (s, 0, 0)),
            ]
            + [pl.BlockSpec((1, 2 * inputs, LANES), lambda s: (s, 0, 0))] * with_rim,
            out_specs=[pl.BlockSpec((1,) + rim_size[1:], lambda s: (s, 0, 0))] * with_rim
            + [
                pl.BlockSpec((size[0], 1) + size[2:], lambda s: (0, s, 0, 0, 0))
                for size in pieces
            ],
            out_shape=[jax.ShapeDtypeStruct(rim_size, jnp.bfloat16)] * with_rim
            + [jax.ShapeDtypeStruct(size, jnp.bfloat16) for size in pieces],
            compiler_params=pltpu.CompilerParams(vmem_limit_bytes=VMEM),
            cost_estimate=pl.CostEstimate(
                flops=12_000_000_000, bytes_accessed=20_000_000, transcendentals=0
            ),
            name="form",
        )(hot, perm, pointing_table, signal, *([rim] if with_rim else []))

    edge, opening = form(groups[:1], signal, rim)
    pieces = [opening]
    if len(groups) > 1:
        later, _ = lax.optimization_barrier((signal, opening))
        pieces += form(groups[1:], later, None)

    mat = synthesis_matrix(filter_taps, inner, reach)

    edge = edge[:, :, :rim_len]
    edge = jnp.concatenate(
        [
            edge[:, 2 * devices * start : 2 * devices * (start + group)].reshape(
                local_subbands, devices, 2 * group * rim_len
            )
            for start, group in zip(starts, groups)
        ],
        axis=2,
    )
    edge = edge.swapaxes(0, 1).reshape(devices, -1)
    edge_size = edge.shape[1]
    planes = -(-edge_size // (2 * groups[0] * LANES))
    edge = jnp.pad(edge, ((0, 0), (0, planes * 2 * groups[0] * LANES - edge_size)))
    edge = edge.reshape(devices, planes, 2 * groups[0], LANES)
    pieces = [
        piece.reshape(devices, local_subbands * inner, 2 * group, LANES)
        for piece, group in zip(pieces, groups)
    ]
    pieces[0] = jnp.concatenate([pieces[0], edge], axis=1)
    got = [lax.all_to_all(p, "sub", split_axis=0, concat_axis=0, tiled=True) for p in pieces]
    edge = got[0][:, local_subbands * inner :].reshape(devices, -1)[:, :edge_size]
    edge = jnp.take(edge.reshape(slots, -1), subband_order, axis=0)
    live_mask = jnp.arange(slots, dtype=jnp.int32) < live_subbands[0]
    edge = jnp.where(live_mask[:, None], edge.astype(jnp.float32), 0.0)

    def edge_of(start, group):
        part = edge[:, 2 * start * rim_len : 2 * (start + group) * rim_len]
        part = part.reshape(bands, chan, 2, group, reach - 1, inner)
        return part.transpose(0, 3, 2, 4, 5, 1).reshape(
            bands, group, 2, reach - 1, inner * chan
        )

    result = None
    for first, start, group, z in zip(firsts, starts, groups, got):
        operands = [subband_order, live_subbands, z, edge_of(start, group), mat]
        in_specs = [
            pl.BlockSpec(memory_space=pl.ANY),
            pl.BlockSpec((1, group, 2, reach - 1, LANES), lambda g, *_: (g, 0, 0, 0, 0)),
            pl.BlockSpec(mat.shape, lambda g, *_: (0, 0)),
        ]
        alias = {}
        if result is not None:
            operands.append(result)
            in_specs.append(pl.BlockSpec(memory_space=pl.ANY))
            alias = {5: 0}
        result = pl.pallas_call(
            functools.partial(synth_kernel, inner, chan, group, reach, local_subbands),
            grid_spec=pltpu.PrefetchScalarGridSpec(
                num_scalar_prefetch=2,
                grid=(bands,),
                in_specs=in_specs,
                out_specs=pl.BlockSpec(
                    (group, 1, 2, local_time * chan), functools.partial(lambda h, g, *_: (h, g, 0, 0), first // group)
                ),
                scratch_shapes=[
                    pltpu.VMEM((2, chan, inner, 2 * group, LANES), jnp.bfloat16),
                    pltpu.VMEM((inner, chan * 2 * group, LANES), jnp.float32),
                    pltpu.VMEM((2, 8 + LANES, LANES), jnp.float32),
                    pltpu.VMEM((group * LANES, mat.shape[0]), jnp.bfloat16),
                    pltpu.VMEM((2, 2 * LANES, LANES), jnp.float32),
                    pltpu.SemaphoreType.DMA((2,)),
                ],
            ),
            out_shape=jax.ShapeDtypeStruct((beam_part, bands, 2, local_time * chan), jnp.bfloat16),
            input_output_aliases=alias,
            compiler_params=pltpu.CompilerParams(vmem_limit_bytes=VMEM),
            cost_estimate=pl.CostEstimate(
                flops=10_000_000_000, bytes_accessed=13_000_000, transcendentals=0
            ),
            name="synth",
        )(*operands)

    return result

MESH = pl.DeviceIdType.MESH


def drain(ref, sem):
    pltpu.make_async_copy(ref, ref, sem).wait()


def relay_kernel(
    n,
    chan,
    order_ref,
    live_ref,
    pick_ref,
    table_ref,
    taps_ref,
    trig_ref,
    volt_ref,
    out_ref,
    z,
    own_out,
    far_out,
    volts,
    far_volts,
    chosen,
    far_chosen,
    own_w,
    far_w,
    lhs,
    stage,
    wide,
    line,
    steps,
    mat,
    made,
    ready,
    tail,
    tail_sent,
    rim,
    z_sem,
    own_sem,
    far_sem,
    in_sem,
    volt_send,
    volt_recv,
    w_send,
    w_recv,
    fwd_send,
    fwd_recv,
    rim_sem,
    out_sem,
):
    f32, bf16 = jnp.float32, jnp.bfloat16
    half, quarter = n // 2, n // 4
    chunks, slots_here, inputs2, _ = volts.shape
    pair = z.shape[2]
    group = pair // 2
    bands = ready.shape[1]
    inner = LANES // chan
    spans = mat.shape[0] // pair_of(chan)
    halo = spans - inner
    blocks = LANES // inner
    ring = far_out.shape[0]

    me, tm = lax.axis_index("sub"), lax.axis_index("tm")
    side, pos = lax.div(me, half), lax.rem(me, half)
    rank, lane = lax.div(pos, quarter), lax.rem(me, quarter)
    other = 1 - side
    is_gate = rank == 1 - side
    near = side
    gate = other * half + side * quarter + lane
    share = slots_here // 2
    mine = pl.ds(tm * share, share)
    theirs = pl.ds((1 - tm) * share, share)

    def chunk_at(step):
        return lax.rem(step + chunks - 1, chunks)

    def source_of(rank_from):
        return other * half + rank_from * quarter + lane

    def load(c):
        return pltpu.make_async_copy(
            volt_ref.at[:, :, pl.ds(pl.multiple_of(c * LANES, LANES), LANES)],
            volts.at[c],
            in_sem.at[c],
        )

    def send_volts(c):
        pltpu.make_async_remote_copy(
            src_ref=volts.at[c],
            dst_ref=far_volts.at[c, rank],
            send_sem=volt_send.at[c],
            recv_sem=volt_recv.at[c, rank],
            device_id=(gate, tm),
            device_id_type=MESH,
        ).start()

    def send_all(sent, src, c, sems):
        def to(j, carry):
            there = lax.rem(pos + 1 + j, half)
            pltpu.make_async_remote_copy(
                src_ref=sent.at[there],
                dst_ref=z.at[c, pl.ds(src * slots_here, slots_here)],
                send_sem=sems.at[there],
                recv_sem=z_sem.at[c, src],
                device_id=(side * half + there, tm),
                device_id_type=MESH,
            ).start()
            return carry

        lax.fori_loop(0, half - 1, to, 0)

    def wait_all(sent, sems):
        def one(j, carry):
            there = lax.rem(pos + 1 + j, half)
            drain(sent.at[there], sems.at[there])
            return carry

        lax.fori_loop(0, half - 1, one, 0)

    def form(weights, signal, sent, src, c):
        def one(s, carry):
            formed = jnp.dot(
                weights[s][:, :inputs2], signal[s], preferred_element_type=f32
            ).astype(bf16)
            for d in range(half):
                sent[d, s] = formed[d * pair : (d + 1) * pair]
            return carry

        lax.fori_loop(0, slots_here, one, 0, unroll=4)

        def keep(s, carry):
            z[c, src * slots_here + s] = sent[pos, s]
            return carry

        lax.fori_loop(0, slots_here, keep, 0)

    def prepare(picked, weights, at):
        w = picked.astype(f32)
        real, imag = w[: inputs2 // 2], w[inputs2 // 2 :]
        rest = jnp.zeros((weights.shape[2] - inputs2, LANES), f32)
        upper = jnp.concatenate([real, -imag, rest], axis=0).T.astype(bf16)
        lower = jnp.concatenate([imag, real, rest], axis=0).T.astype(bf16)
        for d in range(half):
            rows = slice(d * group, (d + 1) * group)
            weights[at, d * pair : d * pair + group] = upper[rows]
            weights[at, d * pair + group : (d + 1) * pair] = lower[rows]

    for step in range(chunks):
        load(chunk_at(step)).start()

    def send_later(step, carry):
        load(chunk_at(step)).wait()
        send_volts(chunk_at(step))
        return carry

    send_later(0, 0)

    pointings = table_ref.shape[2]
    hot = (
        lax.broadcasted_iota(jnp.int32, (pointings, 2 * LANES), 0) == pick_ref[...]
    ).astype(bf16)

    def choose(s, carry):
        picked = jnp.dot(table_ref[s], hot, preferred_element_type=f32).astype(bf16)
        chosen[0, s] = picked[:, :LANES]
        chosen[1, s] = picked[:, LANES:]
        return carry

    lax.fori_loop(0, slots_here, choose, 0)

    def send_weights():
        pltpu.make_async_remote_copy(
            src_ref=chosen.at[other, mine],
            dst_ref=far_chosen.at[rank, mine],
            send_sem=w_send,
            recv_sem=w_recv.at[rank],
            device_id=(gate, tm),
            device_id_type=MESH,
        ).start()

    send_weights()
    lax.fori_loop(1, chunks, send_later, 0)

    def prepare_own(s, carry):
        prepare(chosen[side, s], own_w, s)
        return carry

    lax.fori_loop(0, slots_here, prepare_own, 0)

    for v in range(spans):
        taps = taps_ref[v : v + 1, :]
        mat[v * 2 * chan : (v + 1) * 2 * chan] = (
            jnp.concatenate([taps, taps], axis=1) * trig_ref[...]
        ).astype(bf16)
    tail[...] = jnp.zeros_like(tail)

    def foreign_weights(k):
        forward = pltpu.make_async_remote_copy(
            src_ref=far_chosen.at[k, mine],
            dst_ref=far_chosen.at[k, mine],
            send_sem=fwd_send.at[k],
            recv_sem=fwd_recv.at[k],
            device_id=(me, 1 - tm),
            device_id_type=MESH,
        )
        drain(far_chosen.at[k, mine], w_recv.at[k])
        forward.start()
        drain(far_chosen.at[k, theirs], fwd_recv.at[k])

        def one(s, carry):
            prepare(far_chosen[k, s], far_w.at[k], s)
            return carry

        lax.fori_loop(0, slots_here, one, 0)
        drain(far_chosen.at[k, mine], fwd_send.at[k])

    def foreign(k, i, turn):
        c = chunk_at(i)
        slot = lax.rem(turn, ring)

        @pl.when(i == 0)
        def _():
            foreign_weights(k)

        @pl.when(turn >= ring)
        def _():
            wait_all(far_out.at[slot], far_sem.at[slot])

        drain(far_volts.at[c, k], volt_recv.at[c, k])
        form(far_w.at[k], far_volts.at[c, k], far_out.at[slot], source_of(k), c)
        send_all(far_out.at[slot], source_of(k), c, far_sem.at[slot])

    width = 2 * chan
    fold = LANES // width
    lanes_at = lax.broadcasted_iota(jnp.int32, (LANES // fold, LANES), 1)

    def swap(one, two, size):
        low = lax.rem(lanes_at, 2 * size) < size
        return (
            jnp.where(low, one, pltpu.roll(two, size, 1)),
            jnp.where(low, pltpu.roll(one, LANES - size, 1), two),
        )

    def exchange(parts):
        first, third = swap(parts[0], parts[2], 2 * width)
        second, fourth = swap(parts[1], parts[3], 2 * width)
        return swap(first, second, width) + swap(third, fourth, width)

    def synthesise(i):
        c = chunk_at(lax.rem(i - 1, chunks))

        @pl.when(i <= chunks)
        def _():
            def one(src, carry):
                local = (src == me) | (
                    is_gate & (lax.div(src, half) == other) & (lax.rem(src, quarter) == lane)
                )

                @pl.when(jnp.logical_not(local))
                def _():
                    drain(z.at[c, pl.ds(src * slots_here, slots_here)], z_sem.at[c, src])

                return carry

            lax.fori_loop(0, n, one, 0)

        def copy(s, carry):
            stage[s] = z[c, s]
            return carry

        lax.fori_loop(0, stage.shape[0], copy, 0, unroll=4)

        def gather(g, carry):
            for k in range(chan):
                alive = g * chan + k < live_ref[0]
                block = stage[order_ref[g * chan + k]].astype(f32)
                wide[k * pair : (k + 1) * pair] = jnp.where(alive, block, 0.0)

            for q in range(group // fold):
                rows = [
                    wide[pl.ds(p * group + q * fold + b, chan, stride=pair), :]
                    for b in range(fold)
                    for p in range(2)
                ]
                line[q] = jnp.concatenate(rows, axis=0).T
                split = [line[q, pl.ds(w, LANES // fold, stride=fold), :] for w in range(fold)]
                for b, block in enumerate(exchange(split)):
                    beam = q * fold + b
                    at = g * group + beam
                    steps[beam, :8] = tail[at]
                    steps[beam, 8:] = block
                    tail[at] = block[LANES // fold - 8 :]
                    for e in range(spans // fold):
                        lhs[
                            beam,
                            pl.ds(pl.multiple_of(g * blocks, blocks), blocks),
                            e * LANES : (e + 1) * LANES,
                        ] = steps[
                            beam, pl.ds(8 - halo // fold + e, blocks, stride=inner // fold), :
                        ].astype(bf16)
            return carry

        lax.fori_loop(0, bands, gather, 0)

        out_copy = pltpu.make_async_copy(
            ready,
            out_ref.at[:, :, pl.ds(pl.multiple_of(c * 2 * blocks, 2 * blocks), 2 * blocks)],
            out_sem,
        )

        @pl.when(i > 2)
        def _():
            drain(ready, out_sem)

        def emit(b, carry):
            out = jnp.dot(lhs[b], mat[...], preferred_element_type=f32)
            rows = bands * blocks
            turn = lax.rem(b, 2)
            made[turn, pl.ds(0, rows, stride=2), :] = out[:, :LANES]
            made[turn, pl.ds(1, rows, stride=2), :] = out[:, LANES:]
            for g in range(bands):
                ready[b, g] = made[turn, g * 2 * blocks : (g + 1) * 2 * blocks].astype(bf16)
            return carry

        @pl.when(i > 1)
        def _():
            lax.fori_loop(0, group, emit, 0, unroll=2)
            out_copy.start()

    def pass_tail():
        return pltpu.make_async_remote_copy(
            src_ref=tail_sent,
            dst_ref=rim,
            send_sem=rim_sem.at[0],
            recv_sem=rim_sem.at[1],
            device_id=(me, 1),
            device_id_type=MESH,
        )

    def early(i, carry):
        c = chunk_at(i)

        form(own_w, volts.at[c], own_out.at[c], me, c)
        send_all(own_out.at[c], me, c, own_sem.at[c])

        @pl.when(is_gate)
        def _():
            foreign(1 - near, i, i)

        return carry

    lax.fori_loop(0, chunks, early, 0)

    def step(i, carry):
        @pl.when(is_gate & (i < chunks))
        def _():
            foreign(near, i, chunks + i)

        @pl.when((i == 2) & (tm == 0))
        def _():
            tail[...] = jnp.zeros_like(tail)

        @pl.when((i == 2) & (tm == 1))
        def _():
            drain(rim, rim_sem.at[1])

            def one(j, carry):
                tail[2 * j] = rim[j, :8].astype(f32)
                tail[2 * j + 1] = rim[j, 8:].astype(f32)
                return carry

            lax.fori_loop(0, rim.shape[0], one, 0)

        @pl.when(i >= 1)
        def _():
            synthesise(i)

        @pl.when((i == 1) & (tm == 0))
        def _():
            def one(j, carry):
                pair_at = jnp.concatenate([tail[2 * j], tail[2 * j + 1]], axis=0)
                tail_sent[j] = pair_at.astype(bf16)
                return carry

            lax.fori_loop(0, rim.shape[0], one, 0)
            pass_tail().start()

        return carry

    lax.fori_loop(0, chunks + 2, step, 0)

    drain(ready, out_sem)
    drain(chosen.at[other, mine], w_send)

    @pl.when(tm == 0)
    def _():
        drain(tail_sent, rim_sem.at[0])

    def finish(c, carry):
        drain(volts.at[c], volt_send.at[c])
        wait_all(own_out.at[c], own_sem.at[c])
        return carry

    lax.fori_loop(0, chunks, finish, 0)

    @pl.when(is_gate)
    def _():
        def one(slot, carry):
            wait_all(far_out.at[slot], far_sem.at[slot])
            return carry

        lax.fori_loop(0, ring, one, 0)


def pair_of(chan):
    return 2 * chan


def relay_plan(voltages, pointing_table, beam_pointing, subband_order, live_subbands, filter_taps):
    local, _, inputs, local_time = voltages.shape
    pointings = pointing_table.shape[2]
    beams = beam_pointing.shape[0]
    slots = subband_order.shape[0]
    tap_count, chan = filter_taps.shape
    n = lax.axis_size("sub")
    half = n // 2
    group = beams // n
    pair = 2 * group
    inner = LANES // chan
    spans = inner * (1 + -(-(tap_count - 1) // inner))
    halo = spans - inner
    chunks = local_time // LANES
    bands = slots // chan
    blocks = LANES // inner
    fold = LANES // (2 * chan)
    bf16, f32 = jnp.bfloat16, jnp.float32
    ring = 4

    flat = filter_taps.reshape(-1)
    before, after = (inner - 1) * chan, halo * chan + LANES - flat.shape[0]
    flat = jnp.pad(flat, (before, after))
    taps = jnp.stack(
        [
            flat[before + chan * (halo - v) : before + chan * (halo - v) + LANES]
            for v in range(spans)
        ]
    )
    trig = inverse_table(chan).astype(f32).transpose(2, 3, 0, 1)
    trig = jnp.broadcast_to(trig[:, :, :, None, :], (2, chan, 2, inner, chan))
    trig = trig.reshape(2 * chan, 2 * LANES)
    signal = voltages.reshape(local, 2 * inputs, local_time)
    table = pointing_table.transpose(0, 1, 3, 2).reshape(local, 2 * inputs, pointings)
    lanes_in = 2 * LANES

    vmem = pl.BlockSpec(memory_space=pltpu.VMEM)
    smem = pl.BlockSpec(memory_space=pltpu.SMEM)
    anywhere = pl.BlockSpec(memory_space=pl.ANY)
    dma = pltpu.SemaphoreType.DMA
    out = pl.pallas_call(
        functools.partial(relay_kernel, n, chan),
        in_specs=[smem, smem, vmem, vmem, vmem, vmem, anywhere],
        out_specs=anywhere,
        out_shape=jax.ShapeDtypeStruct((group, bands, 2 * blocks * chunks, LANES), bf16),
        scratch_shapes=[
            pltpu.VMEM((chunks, slots, pair, LANES), bf16),
            pltpu.VMEM((chunks, half, local, pair, LANES), bf16),
            pltpu.VMEM((ring, half, local, pair, LANES), bf16),
            pltpu.VMEM((chunks, local, 2 * inputs, LANES), bf16),
            pltpu.VMEM((chunks, 2, local, 2 * inputs, LANES), bf16),
            pltpu.VMEM((2, local, 2 * inputs, LANES), bf16),
            pltpu.VMEM((2, local, 2 * inputs, LANES), bf16),
            pltpu.VMEM((local, half * pair, lanes_in), bf16),
            pltpu.VMEM((2, local, half * pair, lanes_in), bf16),
            pltpu.VMEM((group, bands * blocks, spans * 2 * chan), bf16),
            pltpu.VMEM((slots, pair, LANES), bf16),
            pltpu.VMEM((chan * pair, LANES), f32),
            pltpu.VMEM((group // fold, LANES, LANES), f32),
            pltpu.VMEM((group, 8 + LANES // fold, LANES), f32),
            pltpu.VMEM((spans * 2 * chan, 2 * LANES), bf16),
            pltpu.VMEM((2, bands * blocks * 2, LANES), f32),
            pltpu.VMEM((group, bands, 2 * blocks, LANES), bf16),
            pltpu.VMEM((bands * group, 8, LANES), f32),
            pltpu.VMEM((bands * group // 2, 16, LANES), bf16),
            pltpu.VMEM((bands * group // 2, 16, LANES), bf16),
            dma((chunks, n)),
            dma((chunks, half)),
            dma((ring, half)),
            dma((chunks,)),
            dma((chunks,)),
            dma((chunks, 2)),
            dma,
            dma((2,)),
            dma((2,)),
            dma((2,)),
            dma((2,)),
            dma,
        ],
        compiler_params=pltpu.CompilerParams(
            vmem_limit_bytes=66_000_000, has_side_effects=True
        ),
        cost_estimate=pl.CostEstimate(
            flops=20_000_000_000, bytes_accessed=20_000_000, transcendentals=0
        ),
        name="relay",
    )(
        subband_order,
        live_subbands,
        beam_pointing.reshape(1, beams),
        table,
        taps,
        trig,
        signal,
    )
    out = out.reshape(group, bands, blocks * chunks, 2, LANES).transpose(0, 1, 3, 2, 4)
    return out.reshape(group, bands, 2, local_time * chan)


def on_device(voltages, pointing_table, beam_pointing, subband_order, live_subbands, filter_taps):
    local, _, inputs, local_time = voltages.shape
    beams = beam_pointing.shape[0]
    tap_count, chan = filter_taps.shape
    n = lax.axis_size("sub")
    fits = (
        lax.axis_size("tm") == 2
        and n % 4 == 0
        and beams == 2 * LANES
        and beams // n % 8 == 0
        and local % 2 == 0
        and local_time % LANES == 0
        and local_time >= 4 * LANES
        and chan * 8 == LANES
        and tap_count <= chan + 1
    )
    plan = relay_plan if fits else direct_plan
    return plan(
        voltages, pointing_table, beam_pointing, subband_order, live_subbands, filter_taps
    )


def solution(mesh):
    in_specs = (P("sub", None, None, "tm"), P("sub", None, None, None), P(), P(), P(), P())
    out_specs = P("sub", None, None, "tm")
    return jax.shard_map(
        on_device, mesh=mesh, in_specs=in_specs, out_specs=out_specs, check_vma=False
    )
```

```python
import functools
import math

import jax
import jax.numpy as jnp
import numpy as np
from jax import lax
from jax.experimental import pallas as pl
from jax.experimental.pallas import tpu as pltpu
from jax.sharding import PartitionSpec as P

LANES = 128
VMEM = 60 * 1024 * 1024


def inverse_table(channel_count):
    channel_index = jnp.arange(channel_count, dtype=jnp.int32)
    phase = (jnp.outer(channel_index, channel_index) % channel_count).astype(jnp.float32) * (
        2.0 * math.pi / channel_count
    )
    cosine = jnp.cos(phase).astype(jnp.bfloat16)
    sine_table = jnp.sin(phase).astype(jnp.bfloat16)
    upper_rows = jnp.stack([cosine, -sine_table], axis=1)
    lower_rows = jnp.stack([sine_table, cosine], axis=1)
    return jnp.stack([upper_rows, lower_rows], axis=0)


def synthesis_matrix(filter_taps, inner, reach):
    tap_count, chan = filter_taps.shape
    table = inverse_table(chan).astype(jnp.float32)
    delta = jnp.arange(reach)[:, None, None]
    tl_in = jnp.arange(inner)[None, :, None]
    tl_out = jnp.arange(inner)[None, None, :]
    tap = inner * delta + tl_out - tl_in
    inside = (tap >= 0) & (tap < tap_count)
    taps = jnp.where(inside[..., None], filter_taps[jnp.clip(tap, 0, tap_count - 1)], 0.0)
    full = (
        taps[:, None, :, None, None, :, :]
        * table.transpose(2, 3, 0, 1)[None, :, None, :, :, None, :]
    )
    return full.reshape(reach * 2 * inner * chan, 2 * inner * chan).astype(jnp.bfloat16)


def form_kernel(inner, groups, with_rim, hot_ref, perm_ref, table_ref, volt_ref, *rest):
    chunks = rest[-len(groups) :]
    f32, bf16 = jnp.float32, jnp.bfloat16
    real, imag = table_ref[0, 0], table_ref[0, 1]
    both = jnp.concatenate(
        [
            jnp.concatenate([real, -imag], axis=1),
            jnp.concatenate([imag, real], axis=1),
        ],
        axis=0,
    )
    weights = jnp.dot(hot_ref[...], both, preferred_element_type=f32).astype(bf16)
    if with_rim:
        rim_ref, rim_out = rest[0], rest[1]
        rim_out[0] = jnp.dot(weights, rim_ref[0], preferred_element_type=f32).astype(bf16)
    signal = jnp.dot(volt_ref[0], perm_ref[...], preferred_element_type=f32).astype(bf16)
    start = 0 if with_rim else hot_ref.shape[0] - 2 * sum(groups) * chunks[0].shape[0]
    for group, out in zip(groups, chunks):
        rows = 2 * group * out.shape[0]
        formed = jnp.dot(
            weights[start : start + rows], signal, preferred_element_type=f32
        ).astype(bf16)
        start += rows
        for d in range(out.shape[0]):
            for tl in range(inner):
                out[d, 0, tl] = formed[
                    2 * d * group : 2 * (d + 1) * group, tl * LANES : (tl + 1) * LANES
                ]


def synth_kernel(
    inner, chan, group, reach, local, order_ref, live_ref, z_ref, rim_ref, mat_ref, *rest
):
    out_ref, held, wide, line, stacked, made, sems = rest[-7:]
    g = pl.program_id(0)
    count = pl.num_programs(0)
    f32, bf16 = jnp.float32, jnp.bfloat16

    def fetch(step, slot):
        named = [order_ref[step * chan + c] for c in range(chan)]
        return [
            pltpu.make_async_copy(
                z_ref.at[lax.div(at, local), pl.ds(lax.rem(at, local) * inner, inner)],
                held.at[slot, c],
                sems.at[slot],
            )
            for c, at in enumerate(named)
        ]

    slot = lax.rem(g, 2)

    @pl.when(g == 0)
    def _():
        for copy in fetch(0, 0):
            copy.start()

    @pl.when(g + 1 < count)
    def _():
        for copy in fetch(g + 1, 1 - slot):
            copy.start()

    for copy in fetch(g, slot):
        copy.wait()

    pair = 2 * group
    for c in range(chan):
        alive = g * chan + c < live_ref[0]
        for tl in range(inner):
            block = held[slot, c, tl].astype(f32)
            wide[tl, c * pair : (c + 1) * pair, :] = jnp.where(alive, block, 0.0)

    width = inner * chan

    def turn(b, carry):
        base = pl.multiple_of(b * LANES, LANES)
        for p in range(2):
            rows = [
                wide[tl, pl.ds(p * group + b, chan, stride=pair), :] for tl in range(inner)
            ]
            line[p, 8 : 8 + LANES, :] = jnp.concatenate(rows, axis=0).T
            line[p, 8 - (reach - 1) : 8, :] = rim_ref[0, b, p]
            for delta in range(reach):
                at = (2 * delta + p) * width
                stacked[pl.ds(base, LANES), at : at + width] = line[
                    p, 8 - delta : 8 - delta + LANES, :
                ].astype(bf16)
        return carry

    lax.fori_loop(0, group, turn, 0, unroll=2)

    def emit(b, carry):
        base = pl.multiple_of(b * 2 * LANES, 2 * LANES)
        out = jnp.dot(
            stacked[pl.ds(base, 2 * LANES), :], mat_ref[...], preferred_element_type=f32
        )
        for i in range(2):
            for q in range(2):
                made[i, q * LANES : (q + 1) * LANES, :] = out[
                    i * LANES : (i + 1) * LANES, q * width : (q + 1) * width
                ]
        for i in range(2):
            for tb in range(LANES):
                both = made[i, pl.ds(tb, 2, stride=LANES), :].astype(bf16)
                out_ref[2 * b + i, 0, :, tb * LANES : (tb + 1) * LANES] = both
        return carry

    lax.fori_loop(0, group // 2, emit, 0)


def direct_plan(voltages, pointing_table, beam_pointing, subband_order, live_subbands, filter_taps):
    local_subbands, _, inputs, local_time = voltages.shape
    pointings = pointing_table.shape[2]
    beam_count = beam_pointing.shape[0]
    slots = subband_order.shape[0]
    tap_count, chan = filter_taps.shape
    inner = LANES // chan
    assert local_time == inner * LANES
    reach = 1 + -(-(tap_count - 1) // inner)
    rim_len = (reach - 1) * inner
    devices = lax.axis_size("sub")
    beam_part = beam_count // devices
    quarter = beam_part // 4
    if beam_part % 8 == 0:
        groups, firsts = [quarter, 2 * quarter, quarter], [0, 2 * quarter, quarter]
    else:
        groups, firsts = [beam_part], [0]
    starts = [sum(groups[:h]) for h in range(len(groups))]
    bands = slots // chan

    signal = voltages.reshape(local_subbands, 2 * inputs, local_time)
    times = range(lax.axis_size("tm"))
    route = [(i - 1, i) for i in times if i > 0]
    rim = lax.ppermute(signal[:, :, local_time - rim_len :], "tm", route)
    rim = jnp.pad(rim, ((0, 0), (0, 0), (0, LANES - rim_len)))

    picks = beam_pointing.reshape(devices, beam_part)
    wanted = jnp.concatenate(
        [
            (
                picks[:, None, first : first + group]
                + pointings * jnp.arange(2, dtype=jnp.int32)[:, None]
            ).reshape(-1)
            for first, group in zip(firsts, groups)
        ]
    )
    hot = (wanted[:, None] == jnp.arange(2 * pointings)[None, :]).astype(jnp.bfloat16)
    source = jnp.arange(local_time, dtype=jnp.int32)
    place = (source % inner) * LANES + source // inner
    perm = (place[:, None] == source[None, :]).astype(jnp.bfloat16)

    def form(groups, signal, rim):
        with_rim = rim is not None
        pieces = [(devices, local_subbands, inner, 2 * group, LANES) for group in groups]
        rim_size = (local_subbands, hot.shape[0], LANES)
        return pl.pallas_call(
            functools.partial(form_kernel, inner, groups, with_rim),
            grid=(local_subbands,),
            in_specs=[
                pl.BlockSpec(hot.shape, lambda s: (0, 0)),
                pl.BlockSpec(perm.shape, lambda s: (0, 0)),
                pl.BlockSpec((1, 2, pointings, inputs), lambda s: (s, 0, 0, 0)),
                pl.BlockSpec((1, 2 * inputs, local_time), lambda s: (s, 0, 0)),
            ]
            + [pl.BlockSpec((1, 2 * inputs, LANES), lambda s: (s, 0, 0))] * with_rim,
            out_specs=[pl.BlockSpec((1,) + rim_size[1:], lambda s: (s, 0, 0))] * with_rim
            + [
                pl.BlockSpec((size[0], 1) + size[2:], lambda s: (0, s, 0, 0, 0))
                for size in pieces
            ],
            out_shape=[jax.ShapeDtypeStruct(rim_size, jnp.bfloat16)] * with_rim
            + [jax.ShapeDtypeStruct(size, jnp.bfloat16) for size in pieces],
            compiler_params=pltpu.CompilerParams(vmem_limit_bytes=VMEM),
            cost_estimate=pl.CostEstimate(
                flops=12_000_000_000, bytes_accessed=20_000_000, transcendentals=0
            ),
            name="form",
        )(hot, perm, pointing_table, signal, *([rim] if with_rim else []))

    edge, opening = form(groups[:1], signal, rim)
    pieces = [opening]
    if len(groups) > 1:
        later, _ = lax.optimization_barrier((signal, opening))
        pieces += form(groups[1:], later, None)

    mat = synthesis_matrix(filter_taps, inner, reach)

    edge = edge[:, :, :rim_len]
    edge = jnp.concatenate(
        [
            edge[:, 2 * devices * start : 2 * devices * (start + group)].reshape(
                local_subbands, devices, 2 * group * rim_len
            )
            for start, group in zip(starts, groups)
        ],
        axis=2,
    )
    edge = edge.swapaxes(0, 1).reshape(devices, -1)
    edge_size = edge.shape[1]
    planes = -(-edge_size // (2 * groups[0] * LANES))
    edge = jnp.pad(edge, ((0, 0), (0, planes * 2 * groups[0] * LANES - edge_size)))
    edge = edge.reshape(devices, planes, 2 * groups[0], LANES)
    pieces = [
        piece.reshape(devices, local_subbands * inner, 2 * group, LANES)
        for piece, group in zip(pieces, groups)
    ]
    pieces[0] = jnp.concatenate([pieces[0], edge], axis=1)
    got = [lax.all_to_all(p, "sub", split_axis=0, concat_axis=0, tiled=True) for p in pieces]
    edge = got[0][:, local_subbands * inner :].reshape(devices, -1)[:, :edge_size]
    edge = jnp.take(edge.reshape(slots, -1), subband_order, axis=0)
    live_mask = jnp.arange(slots, dtype=jnp.int32) < live_subbands[0]
    edge = jnp.where(live_mask[:, None], edge.astype(jnp.float32), 0.0)

    def edge_of(start, group):
        part = edge[:, 2 * start * rim_len : 2 * (start + group) * rim_len]
        part = part.reshape(bands, chan, 2, group, reach - 1, inner)
        return part.transpose(0, 3, 2, 4, 5, 1).reshape(
            bands, group, 2, reach - 1, inner * chan
        )

    result = None
    for first, start, group, z in zip(firsts, starts, groups, got):
        operands = [subband_order, live_subbands, z, edge_of(start, group), mat]
        in_specs = [
            pl.BlockSpec(memory_space=pl.ANY),
            pl.BlockSpec((1, group, 2, reach - 1, LANES), lambda g, *_: (g, 0, 0, 0, 0)),
            pl.BlockSpec(mat.shape, lambda g, *_: (0, 0)),
        ]
        alias = {}
        if result is not None:
            operands.append(result)
            in_specs.append(pl.BlockSpec(memory_space=pl.ANY))
            alias = {5: 0}
        result = pl.pallas_call(
            functools.partial(synth_kernel, inner, chan, group, reach, local_subbands),
            grid_spec=pltpu.PrefetchScalarGridSpec(
                num_scalar_prefetch=2,
                grid=(bands,),
                in_specs=in_specs,
                out_specs=pl.BlockSpec(
                    (group, 1, 2, local_time * chan), functools.partial(lambda h, g, *_: (h, g, 0, 0), first // group)
                ),
                scratch_shapes=[
                    pltpu.VMEM((2, chan, inner, 2 * group, LANES), jnp.bfloat16),
                    pltpu.VMEM((inner, chan * 2 * group, LANES), jnp.float32),
                    pltpu.VMEM((2, 8 + LANES, LANES), jnp.float32),
                    pltpu.VMEM((group * LANES, mat.shape[0]), jnp.bfloat16),
                    pltpu.VMEM((2, 2 * LANES, LANES), jnp.float32),
                    pltpu.SemaphoreType.DMA((2,)),
                ],
            ),
            out_shape=jax.ShapeDtypeStruct((beam_part, bands, 2, local_time * chan), jnp.bfloat16),
            input_output_aliases=alias,
            compiler_params=pltpu.CompilerParams(vmem_limit_bytes=VMEM),
            cost_estimate=pl.CostEstimate(
                flops=10_000_000_000, bytes_accessed=13_000_000, transcendentals=0
            ),
            name="synth",
        )(*operands)

    return result

MESH = pl.DeviceIdType.MESH


def drain(ref, sem):
    pltpu.make_async_copy(ref, ref, sem).wait()


def relay_kernel(
    n,
    chan,
    order_ref,
    live_ref,
    pick_ref,
    table_ref,
    taps_ref,
    trig_ref,
    volt_ref,
    out_ref,
    z,
    own_out,
    far_out,
    volts,
    far_volts,
    chosen,
    far_chosen,
    own_w,
    far_w,
    lhs,
    stage,
    wide,
    select,
    steps,
    mat,
    made,
    ready,
    tail,
    tail_sent,
    rim,
    head,
    joint,
    redo,
    mended,
    z_sem,
    own_sem,
    far_sem,
    in_sem,
    volt_send,
    volt_recv,
    w_send,
    w_recv,
    fwd_send,
    fwd_recv,
    rim_sem,
    out_sem,
    mend_sem,
):
    f32, bf16 = jnp.float32, jnp.bfloat16
    half, quarter = n // 2, n // 4
    chunks, slots_here, inputs2, _ = volts.shape
    pair = z.shape[2]
    group = pair // 2
    bands = ready.shape[1]
    inner = LANES // chan
    spans = mat.shape[0] // pair_of(chan)
    halo = spans - inner
    blocks = LANES // inner
    ring = far_out.shape[0]
    pitch = wide.shape[0] // chan
    parts = volt_recv.shape[2]
    batch = slots_here // parts
    unroll = math.gcd(batch, 6)

    me, tm = lax.axis_index("sub"), lax.axis_index("tm")
    side, pos = lax.div(me, half), lax.rem(me, half)
    rank, lane = lax.div(pos, quarter), lax.rem(me, quarter)
    other = 1 - side
    is_gate = rank == 1 - side
    near = side
    gate = other * half + side * quarter + lane
    share = slots_here // 2
    mine = pl.ds(tm * share, share)
    theirs = pl.ds((1 - tm) * share, share)

    def chunk_at(step):
        return lax.rem(step + chunks - 1, chunks)

    def source_of(rank_from):
        return other * half + rank_from * quarter + lane

    def load(c):
        return pltpu.make_async_copy(
            volt_ref.at[:, :, pl.ds(pl.multiple_of(c * LANES, LANES), LANES)],
            volts.at[c],
            in_sem.at[c],
        )

    def send_volts(c):
        for part in range(parts):
            some = pl.ds(part * batch, batch)
            pltpu.make_async_remote_copy(
                src_ref=volts.at[c, some],
                dst_ref=far_volts.at[c, rank, some],
                send_sem=volt_send.at[c],
                recv_sem=volt_recv.at[c, rank, part],
                device_id=(gate, tm),
                device_id_type=MESH,
            ).start()

    def send_all(sent, src, c, sems, first, count):
        def to(j, carry):
            there = lax.rem(pos + 1 + j, half)
            pltpu.make_async_remote_copy(
                src_ref=sent.at[there, pl.ds(first, count)],
                dst_ref=z.at[c, pl.ds(src * slots_here + first, count)],
                send_sem=sems.at[there],
                recv_sem=z_sem.at[c, src],
                device_id=(side * half + there, tm),
                device_id_type=MESH,
            ).start()
            return carry

        lax.fori_loop(0, half - 1, to, 0)

    def wait_all(sent, sems):
        def one(j, carry):
            there = lax.rem(pos + 1 + j, half)
            drain(sent.at[there], sems.at[there])
            return carry

        lax.fori_loop(0, half - 1, one, 0)

    def form(weights, signal, sent, src, c, first, count):
        def one(j, carry):
            s = first + j
            formed = jnp.dot(
                weights[s][:, :inputs2], signal[s], preferred_element_type=f32
            ).astype(bf16)
            for d in range(half):
                sent[d, s] = formed[d * pair : (d + 1) * pair]
            return carry

        lax.fori_loop(0, count, one, 0, unroll=unroll)

    def keep(sent, src, c):
        def one(s, carry):
            z[c, src * slots_here + s] = sent[pos, s]
            return carry

        lax.fori_loop(0, slots_here, one, 0, unroll=unroll)

    def prepare(picked, weights, at):
        w = picked.astype(f32)
        real, imag = w[: inputs2 // 2], w[inputs2 // 2 :]
        rest = jnp.zeros((weights.shape[2] - inputs2, LANES), f32)
        upper = jnp.concatenate([real, -imag, rest], axis=0).T.astype(bf16)
        lower = jnp.concatenate([imag, real, rest], axis=0).T.astype(bf16)
        for d in range(half):
            rows = slice(d * group, (d + 1) * group)
            weights[at, d * pair : d * pair + group] = upper[rows]
            weights[at, d * pair + group : (d + 1) * pair] = lower[rows]

    load(chunk_at(0)).start()

    def send_later(step, carry):
        load(chunk_at(step)).wait()
        send_volts(chunk_at(step))
        return carry

    send_later(0, 0)
    for step in range(1, chunks):
        load(chunk_at(step)).start()

    pointings = table_ref.shape[2]
    hot = (
        lax.broadcasted_iota(jnp.int32, (pointings, 2 * LANES), 0) == pick_ref[...]
    ).astype(bf16)

    def choose(s, carry):
        picked = jnp.dot(table_ref[s], hot, preferred_element_type=f32).astype(bf16)
        chosen[0, s] = picked[:, :LANES]
        chosen[1, s] = picked[:, LANES:]
        return carry

    lax.fori_loop(0, slots_here, choose, 0)

    def send_weights():
        pltpu.make_async_remote_copy(
            src_ref=chosen.at[other, mine],
            dst_ref=far_chosen.at[rank, mine],
            send_sem=w_send,
            recv_sem=w_recv.at[rank],
            device_id=(gate, tm),
            device_id_type=MESH,
        ).start()

    send_weights()
    lax.fori_loop(1, chunks, send_later, 0)

    def prepare_own(s, carry):
        prepare(chosen[side, s], own_w, s)
        return carry

    lax.fori_loop(0, slots_here, prepare_own, 0)

    tap_count = taps_ref.shape[0]
    repeat = lax.broadcasted_iota(jnp.int32, (chan, LANES), 0) == lax.rem(
        lax.broadcasted_iota(jnp.int32, (chan, LANES), 1), chan
    )
    taps = jnp.dot(
        taps_ref[...],
        repeat.astype(f32),
        precision=lax.Precision.HIGHEST,
        preferred_element_type=f32,
    )
    tap_at = lax.broadcasted_iota(jnp.int32, (tap_count, LANES), 0)
    time_at = lax.div(lax.broadcasted_iota(jnp.int32, (tap_count, LANES), 1), chan)
    for v in range(spans):
        row = jnp.sum(
            jnp.where(time_at - tap_at == v - halo, taps, 0.0), axis=0, keepdims=True
        )
        mat[v * 2 * chan : (v + 1) * 2 * chan] = (
            jnp.concatenate([row, row], axis=1) * trig_ref[...]
        ).astype(bf16)
    select_row = lax.broadcasted_iota(jnp.int32, (LANES, LANES), 0)
    phases = LANES // (2 * chan)
    select_time = lax.rem(select_row, LANES // phases) * phases + lax.div(
        select_row, LANES // phases
    )
    select[...] = (
        lax.broadcasted_iota(jnp.int32, (LANES, LANES), 1) == select_time
    ).astype(bf16)
    tail[...] = jnp.zeros_like(tail)

    def foreign_weights(k):
        forward = pltpu.make_async_remote_copy(
            src_ref=far_chosen.at[k, mine],
            dst_ref=far_chosen.at[k, mine],
            send_sem=fwd_send.at[k],
            recv_sem=fwd_recv.at[k],
            device_id=(me, 1 - tm),
            device_id_type=MESH,
        )
        drain(far_chosen.at[k, mine], w_recv.at[k])
        forward.start()
        drain(far_chosen.at[k, theirs], fwd_recv.at[k])

        def one(s, carry):
            prepare(far_chosen[k, s], far_w.at[k], s)
            return carry

        lax.fori_loop(0, slots_here, one, 0)
        drain(far_chosen.at[k, mine], fwd_send.at[k])

    def foreign(k, i, turn):
        c = chunk_at(i)
        slot = lax.rem(turn, ring)

        @pl.when(i == 0)
        def _():
            foreign_weights(k)

        @pl.when(turn >= ring)
        def _():
            wait_all(far_out.at[slot], far_sem.at[slot])

        src = source_of(k)

        def one(part, carry):
            first = part * batch
            drain(far_volts.at[c, k, pl.ds(first, batch)], volt_recv.at[c, k, part])
            form(far_w.at[k], far_volts.at[c, k], far_out.at[slot], src, c, first, batch)
            send_all(far_out.at[slot], src, c, far_sem.at[slot], first, batch)
            return carry

        lax.fori_loop(0, parts, one, 0)
        keep(far_out.at[slot], src, c)

    width = 2 * chan
    fold = LANES // width
    lanes_at = lax.broadcasted_iota(jnp.int32, (LANES // fold, LANES), 1)

    def swap(one, two, size):
        low = lax.rem(lanes_at, 2 * size) < size
        return (
            jnp.where(low, one, pltpu.roll(two, size, 1)),
            jnp.where(low, pltpu.roll(one, LANES - size, 1), two),
        )

    def exchange(parts):
        first, third = swap(parts[0], parts[2], 2 * width)
        second, fourth = swap(parts[1], parts[3], 2 * width)
        return swap(first, second, width) + swap(third, fourth, width)

    def synthesise(i):
        c = chunk_at(i - 1)

        def one(src, carry):
            local = (src == me) | (
                is_gate & (lax.div(src, half) == other) & (lax.rem(src, quarter) == lane)
            )

            @pl.when(jnp.logical_not(local))
            def _():
                drain(z.at[c, pl.ds(src * slots_here, slots_here)], z_sem.at[c, src])

            return carry

        lax.fori_loop(0, n, one, 0)

        def copy(s, carry):
            stage[s] = z[c, s]
            return carry

        lax.fori_loop(0, stage.shape[0], copy, 0, unroll=4)

        def gather(g, carry):
            for k in range(chan):
                alive = g * chan + k < live_ref[0]
                block = stage[order_ref[g * chan + k]].astype(f32)
                wide[k * pitch : k * pitch + pair] = jnp.where(alive, block, 0.0)

            for q in range(group // fold):
                rows = [
                    wide[pl.ds(p * group + q * fold + b, chan, stride=pitch), :]
                    for b in range(fold)
                    for p in range(2)
                ]
                turned = lax.dot_general(
                    select[...],
                    jnp.concatenate(rows, axis=0).astype(bf16),
                    (((1,), (1,)), ((), ())),
                    preferred_element_type=f32,
                )
                size = LANES // fold
                split = [turned[w * size : (w + 1) * size] for w in range(fold)]
                for b, block in enumerate(exchange(split)):
                    beam = q * fold + b
                    at = g * group + beam
                    steps[beam, :8] = tail[at]
                    steps[beam, 8:] = block
                    tail[at] = block[LANES // fold - 8 :]
                    head[lax.min(i - 1, 1), at] = block[:8]
                    for e in range(spans // fold):
                        lhs[e, beam, pl.ds(pl.multiple_of(g * blocks, blocks), blocks)] = steps[
                            beam, pl.ds(8 - halo // fold + e, blocks, stride=inner // fold), :
                        ].astype(bf16)
            return carry

        lax.fori_loop(0, bands, gather, 0)

        out_copy = pltpu.make_async_copy(
            ready,
            out_ref.at[:, :, pl.ds(pl.multiple_of(c * 2 * blocks, 2 * blocks), 2 * blocks)],
            out_sem,
        )

        @pl.when(i > 1)
        def _():
            drain(ready, out_sem)

        def emit(b, carry):
            rows = bands * blocks
            terms = [
                lhs[e, pl.ds(b * fold, fold)].reshape(fold * rows, LANES)
                for e in range(spans // fold)
            ]
            out = jnp.dot(
                jnp.concatenate(terms, axis=1), mat[...], preferred_element_type=f32
            )
            made[pl.ds(0, fold * rows, stride=2), :] = out[:, :LANES]
            made[pl.ds(1, fold * rows, stride=2), :] = out[:, LANES:]
            for j in range(fold):
                for g in range(bands):
                    at = (j * bands + g) * 2 * blocks
                    ready[b * fold + j, g] = made[at : at + 2 * blocks].astype(bf16)
            return carry

        lax.fori_loop(0, group // fold, emit, 0)
        out_copy.start()

    def patch():
        rows = halo // inner + 2
        opening = bands * rows

        def restack(b, carry):
            for g in range(bands):
                at = g * group + b
                joint[g, :8] = tail[at]
                joint[g, 8:] = head[0, at]
                for e in range(spans // fold):
                    redo[e, b, g * rows : (g + 1) * rows] = joint[
                        g, pl.ds(8 - halo // fold + e, rows, stride=inner // fold), :
                    ]
            return carry

        lax.fori_loop(0, group, restack, 0)
        terms = [
            redo[e].reshape(group * opening, LANES).astype(bf16) for e in range(spans // fold)
        ]
        out = jnp.dot(jnp.concatenate(terms, axis=1), mat[...], preferred_element_type=f32)
        made[pl.ds(0, group * opening, stride=2), :] = out[:, :LANES]
        made[pl.ds(1, group * opening, stride=2), :] = out[:, LANES:]

        def place(b, carry):
            for g in range(bands):
                at = pl.multiple_of(b * opening * 2 + g * rows * 2, rows * 2)
                mended[b, g] = made[pl.ds(at, rows * 2)].astype(bf16)
            return carry

        lax.fori_loop(0, group, place, 0)
        c = chunk_at(0)
        start = pl.multiple_of(c * 2 * blocks, 2 * blocks)
        copy = pltpu.make_async_copy(
            mended, out_ref.at[:, :, pl.ds(start, rows * 2)], mend_sem
        )
        copy.start()
        copy.wait()

    def pass_tail():
        return pltpu.make_async_remote_copy(
            src_ref=tail_sent,
            dst_ref=rim,
            send_sem=rim_sem.at[0],
            recv_sem=rim_sem.at[1],
            device_id=(me, 1),
            device_id_type=MESH,
        )

    def early(i, carry):
        c = chunk_at(i)

        form(own_w, volts.at[c], own_out.at[c], me, c, 0, slots_here)
        send_all(own_out.at[c], me, c, own_sem.at[c], 0, slots_here)
        keep(own_out.at[c], me, c)

        @pl.when(is_gate)
        def _():
            foreign(1 - near, i, i)

        return carry

    lax.fori_loop(0, chunks, early, 0)

    def step(i, carry):
        @pl.when(is_gate & (i < chunks))
        def _():
            foreign(near, i, chunks + i)

        @pl.when((i == 2) & (tm == 0))
        def _():
            tail[...] = jnp.zeros_like(tail)

        @pl.when((i == 2) & (tm == 1))
        def _():
            drain(rim, rim_sem.at[1])

            def one(j, carry):
                tail[2 * j] = rim[j, :8].astype(f32)
                tail[2 * j + 1] = rim[j, 8:].astype(f32)
                return carry

            lax.fori_loop(0, rim.shape[0], one, 0)

        @pl.when(i >= 1)
        def _():
            synthesise(i)

        @pl.when((i == 1) & (tm == 0))
        def _():
            def one(j, carry):
                pair_at = jnp.concatenate([tail[2 * j], tail[2 * j + 1]], axis=0)
                tail_sent[j] = pair_at.astype(bf16)
                return carry

            lax.fori_loop(0, rim.shape[0], one, 0)
            pass_tail().start()

        return carry

    lax.fori_loop(0, chunks + 1, step, 0)
    patch()

    drain(ready, out_sem)
    drain(chosen.at[other, mine], w_send)

    @pl.when(tm == 0)
    def _():
        drain(tail_sent, rim_sem.at[0])

    def finish(c, carry):
        drain(volts.at[c], volt_send.at[c])
        wait_all(own_out.at[c], own_sem.at[c])
        return carry

    lax.fori_loop(0, chunks, finish, 0)

    @pl.when(is_gate)
    def _():
        def one(slot, carry):
            wait_all(far_out.at[slot], far_sem.at[slot])
            return carry

        lax.fori_loop(0, ring, one, 0)


def hand_over_kernel(in_ref, out_ref, held, in_sem, out_sem):
    count = held.shape[0]
    reads = [pltpu.make_async_copy(in_ref.at[b], held.at[b], in_sem.at[b]) for b in range(count)]
    writes = [
        pltpu.make_async_copy(held.at[b], out_ref.at[b], out_sem.at[b]) for b in range(count)
    ]
    for read in reads:
        read.start()
    for read, write in zip(reads, writes):
        read.wait()
        write.start()
    for write in writes:
        write.wait()


def pair_of(chan):
    return 2 * chan


def relay_plan(voltages, pointing_table, beam_pointing, subband_order, live_subbands, filter_taps):
    local, _, inputs, local_time = voltages.shape
    pointings = pointing_table.shape[2]
    beams = beam_pointing.shape[0]
    slots = subband_order.shape[0]
    tap_count, chan = filter_taps.shape
    n = lax.axis_size("sub")
    half = n // 2
    group = beams // n
    pair = 2 * group
    inner = LANES // chan
    spans = inner * (1 + -(-(tap_count - 1) // inner))
    halo = spans - inner
    chunks = local_time // LANES
    bands = slots // chan
    blocks = LANES // inner
    fold = LANES // (2 * chan)
    bf16, f32 = jnp.bfloat16, jnp.float32
    ring = 4

    at = np.arange(chan)
    phase = (np.outer(at, at) % chan).astype(np.float32) * np.float32(2.0 * math.pi / chan)
    cosine, sine = (
        np.asarray(f(phase), jnp.bfloat16).astype(np.float32) for f in (np.cos, np.sin)
    )
    trig = np.stack([np.stack([cosine, -sine], 1), np.stack([sine, cosine], 1)])
    trig = trig.transpose(2, 3, 0, 1)[:, :, :, None, :]
    trig = np.broadcast_to(trig, (2, chan, 2, inner, chan))
    trig = jnp.asarray(trig.reshape(2 * chan, 2 * LANES))
    signal = voltages.reshape(local, 2 * inputs, local_time)
    table = pointing_table.transpose(0, 1, 3, 2).reshape(local, 2 * inputs, pointings)
    lanes_in = 2 * LANES

    vmem = pl.BlockSpec(memory_space=pltpu.VMEM)
    smem = pl.BlockSpec(memory_space=pltpu.SMEM)
    anywhere = pl.BlockSpec(memory_space=pl.ANY)
    dma = pltpu.SemaphoreType.DMA
    out = pl.pallas_call(
        functools.partial(relay_kernel, n, chan),
        in_specs=[smem, smem, vmem, vmem, vmem, vmem, anywhere],
        out_specs=anywhere,
        out_shape=jax.ShapeDtypeStruct((group, bands, 2 * blocks * chunks, LANES), bf16),
        scratch_shapes=[
            pltpu.VMEM((chunks, slots, pair, LANES), bf16),
            pltpu.VMEM((chunks, half, local, pair, LANES), bf16),
            pltpu.VMEM((ring, half, local, pair, LANES), bf16),
            pltpu.VMEM((chunks, local, 2 * inputs, LANES), bf16),
            pltpu.VMEM((chunks, 2, local, 2 * inputs, LANES), bf16),
            pltpu.VMEM((2, local, 2 * inputs, LANES), bf16),
            pltpu.VMEM((2, local, 2 * inputs, LANES), bf16),
            pltpu.VMEM((local, half * pair, lanes_in), bf16),
            pltpu.VMEM((2, local, half * pair, lanes_in), bf16),
            pltpu.VMEM((spans // fold, group, bands * blocks, LANES), bf16),
            pltpu.VMEM((slots, pair, LANES), bf16),
            pltpu.VMEM((chan * (pair + 1), LANES), f32),
            pltpu.VMEM((LANES, LANES), bf16),
            pltpu.VMEM((group, 8 + LANES // fold, LANES), f32),
            pltpu.VMEM((spans * 2 * chan, 2 * LANES), bf16),
            pltpu.VMEM((fold * bands * blocks * 2, LANES), f32),
            pltpu.VMEM((group, bands, 2 * blocks, LANES), bf16),
            pltpu.VMEM((bands * group, 8, LANES), f32),
            pltpu.VMEM((bands * group // 2, 16, LANES), bf16),
            pltpu.VMEM((bands * group // 2, 16, LANES), bf16),
            pltpu.VMEM((2, bands * group, 8, LANES), f32),
            pltpu.VMEM((bands, 16, LANES), f32),
            pltpu.VMEM((spans // fold, group, bands * (halo // inner + 2), LANES), f32),
            pltpu.VMEM((group, bands, 2 * (halo // inner + 2), LANES), bf16),
            dma((chunks, n)),
            dma((chunks, half)),
            dma((ring, half)),
            dma((chunks,)),
            dma((chunks,)),
            dma((chunks, 2, 1)),
            dma,
            dma((2,)),
            dma((2,)),
            dma((2,)),
            dma((2,)),
            dma,
            dma,
        ],
        compiler_params=pltpu.CompilerParams(
            vmem_limit_bytes=66_000_000, has_side_effects=True
        ),
        cost_estimate=pl.CostEstimate(
            flops=20_000_000_000, bytes_accessed=20_000_000, transcendentals=0
        ),
        name="relay",
    )(
        subband_order,
        live_subbands,
        beam_pointing.reshape(1, beams),
        table,
        filter_taps,
        trig,
        signal,
    )
    out = pl.pallas_call(
        hand_over_kernel,
        in_specs=[anywhere],
        out_specs=anywhere,
        out_shape=jax.ShapeDtypeStruct(out.shape, bf16),
        scratch_shapes=[pltpu.VMEM(out.shape, bf16), dma((group,)), dma((group,))],
        compiler_params=pltpu.CompilerParams(vmem_limit_bytes=VMEM),
        name="hand_over",
    )(out)
    out = out.reshape(group, bands, blocks * chunks, 2, LANES).transpose(0, 1, 3, 2, 4)
    return out.reshape(group, bands, 2, local_time * chan)


def on_device(voltages, pointing_table, beam_pointing, subband_order, live_subbands, filter_taps):
    local, _, inputs, local_time = voltages.shape
    beams = beam_pointing.shape[0]
    tap_count, chan = filter_taps.shape
    n = lax.axis_size("sub")
    fits = (
        lax.axis_size("tm") == 2
        and n % 4 == 0
        and beams == 2 * LANES
        and beams // n % 8 == 0
        and local % 2 == 0
        and local_time % LANES == 0
        and local_time >= 4 * LANES
        and chan * 8 == LANES
        and tap_count <= chan + 1
    )
    plan = relay_plan if fits else direct_plan
    return plan(
        voltages, pointing_table, beam_pointing, subband_order, live_subbands, filter_taps
    )


def solution(mesh):
    in_specs = (P("sub", None, None, "tm"), P("sub", None, None, None), P(), P(), P(), P())
    out_specs = P("sub", None, None, "tm")
    return jax.shard_map(
        on_device, mesh=mesh, in_specs=in_specs, out_specs=out_specs, check_vma=False
    )
```

```python
import functools
import math

import jax
import jax.numpy as jnp
import numpy as np
from jax import lax
from jax.experimental import pallas as pl
from jax.experimental.pallas import tpu as pltpu
from jax.sharding import PartitionSpec as P

LANES = 128
VMEM = 60 * 1024 * 1024


def inverse_table(channel_count):
    channel_index = jnp.arange(channel_count, dtype=jnp.int32)
    phase = (jnp.outer(channel_index, channel_index) % channel_count).astype(jnp.float32) * (
        2.0 * math.pi / channel_count
    )
    cosine = jnp.cos(phase).astype(jnp.bfloat16)
    sine_table = jnp.sin(phase).astype(jnp.bfloat16)
    upper_rows = jnp.stack([cosine, -sine_table], axis=1)
    lower_rows = jnp.stack([sine_table, cosine], axis=1)
    return jnp.stack([upper_rows, lower_rows], axis=0)


def synthesis_matrix(filter_taps, inner, reach):
    tap_count, chan = filter_taps.shape
    table = inverse_table(chan).astype(jnp.float32)
    delta = jnp.arange(reach)[:, None, None]
    tl_in = jnp.arange(inner)[None, :, None]
    tl_out = jnp.arange(inner)[None, None, :]
    tap = inner * delta + tl_out - tl_in
    inside = (tap >= 0) & (tap < tap_count)
    taps = jnp.where(inside[..., None], filter_taps[jnp.clip(tap, 0, tap_count - 1)], 0.0)
    full = (
        taps[:, None, :, None, None, :, :]
        * table.transpose(2, 3, 0, 1)[None, :, None, :, :, None, :]
    )
    return full.reshape(reach * 2 * inner * chan, 2 * inner * chan).astype(jnp.bfloat16)


def form_kernel(inner, groups, with_rim, hot_ref, perm_ref, table_ref, volt_ref, *rest):
    chunks = rest[-len(groups) :]
    f32, bf16 = jnp.float32, jnp.bfloat16
    real, imag = table_ref[0, 0], table_ref[0, 1]
    both = jnp.concatenate(
        [
            jnp.concatenate([real, -imag], axis=1),
            jnp.concatenate([imag, real], axis=1),
        ],
        axis=0,
    )
    weights = jnp.dot(hot_ref[...], both, preferred_element_type=f32).astype(bf16)
    if with_rim:
        rim_ref, rim_out = rest[0], rest[1]
        rim_out[0] = jnp.dot(weights, rim_ref[0], preferred_element_type=f32).astype(bf16)
    signal = jnp.dot(volt_ref[0], perm_ref[...], preferred_element_type=f32).astype(bf16)
    start = 0 if with_rim else hot_ref.shape[0] - 2 * sum(groups) * chunks[0].shape[0]
    for group, out in zip(groups, chunks):
        rows = 2 * group * out.shape[0]
        formed = jnp.dot(
            weights[start : start + rows], signal, preferred_element_type=f32
        ).astype(bf16)
        start += rows
        for d in range(out.shape[0]):
            for tl in range(inner):
                out[d, 0, tl] = formed[
                    2 * d * group : 2 * (d + 1) * group, tl * LANES : (tl + 1) * LANES
                ]


def synth_kernel(
    inner, chan, group, reach, local, order_ref, live_ref, z_ref, rim_ref, mat_ref, *rest
):
    out_ref, held, wide, line, stacked, made, sems = rest[-7:]
    g = pl.program_id(0)
    count = pl.num_programs(0)
    f32, bf16 = jnp.float32, jnp.bfloat16

    def fetch(step, slot):
        named = [order_ref[step * chan + c] for c in range(chan)]
        return [
            pltpu.make_async_copy(
                z_ref.at[lax.div(at, local), pl.ds(lax.rem(at, local) * inner, inner)],
                held.at[slot, c],
                sems.at[slot],
            )
            for c, at in enumerate(named)
        ]

    slot = lax.rem(g, 2)

    @pl.when(g == 0)
    def _():
        for copy in fetch(0, 0):
            copy.start()

    @pl.when(g + 1 < count)
    def _():
        for copy in fetch(g + 1, 1 - slot):
            copy.start()

    for copy in fetch(g, slot):
        copy.wait()

    pair = 2 * group
    for c in range(chan):
        alive = g * chan + c < live_ref[0]
        for tl in range(inner):
            block = held[slot, c, tl].astype(f32)
            wide[tl, c * pair : (c + 1) * pair, :] = jnp.where(alive, block, 0.0)

    width = inner * chan

    def turn(b, carry):
        base = pl.multiple_of(b * LANES, LANES)
        for p in range(2):
            rows = [
                wide[tl, pl.ds(p * group + b, chan, stride=pair), :] for tl in range(inner)
            ]
            line[p, 8 : 8 + LANES, :] = jnp.concatenate(rows, axis=0).T
            line[p, 8 - (reach - 1) : 8, :] = rim_ref[0, b, p]
            for delta in range(reach):
                at = (2 * delta + p) * width
                stacked[pl.ds(base, LANES), at : at + width] = line[
                    p, 8 - delta : 8 - delta + LANES, :
                ].astype(bf16)
        return carry

    lax.fori_loop(0, group, turn, 0, unroll=2)

    def emit(b, carry):
        base = pl.multiple_of(b * 2 * LANES, 2 * LANES)
        out = jnp.dot(
            stacked[pl.ds(base, 2 * LANES), :], mat_ref[...], preferred_element_type=f32
        )
        for i in range(2):
            for q in range(2):
                made[i, q * LANES : (q + 1) * LANES, :] = out[
                    i * LANES : (i + 1) * LANES, q * width : (q + 1) * width
                ]
        for i in range(2):
            for tb in range(LANES):
                both = made[i, pl.ds(tb, 2, stride=LANES), :].astype(bf16)
                out_ref[2 * b + i, 0, :, tb * LANES : (tb + 1) * LANES] = both
        return carry

    lax.fori_loop(0, group // 2, emit, 0)


def direct_plan(voltages, pointing_table, beam_pointing, subband_order, live_subbands, filter_taps):
    local_subbands, _, inputs, local_time = voltages.shape
    pointings = pointing_table.shape[2]
    beam_count = beam_pointing.shape[0]
    slots = subband_order.shape[0]
    tap_count, chan = filter_taps.shape
    inner = LANES // chan
    assert local_time == inner * LANES
    reach = 1 + -(-(tap_count - 1) // inner)
    rim_len = (reach - 1) * inner
    devices = lax.axis_size("sub")
    beam_part = beam_count // devices
    quarter = beam_part // 4
    if beam_part % 8 == 0:
        groups, firsts = [quarter, 2 * quarter, quarter], [0, 2 * quarter, quarter]
    else:
        groups, firsts = [beam_part], [0]
    starts = [sum(groups[:h]) for h in range(len(groups))]
    bands = slots // chan

    signal = voltages.reshape(local_subbands, 2 * inputs, local_time)
    times = range(lax.axis_size("tm"))
    route = [(i - 1, i) for i in times if i > 0]
    rim = lax.ppermute(signal[:, :, local_time - rim_len :], "tm", route)
    rim = jnp.pad(rim, ((0, 0), (0, 0), (0, LANES - rim_len)))

    picks = beam_pointing.reshape(devices, beam_part)
    wanted = jnp.concatenate(
        [
            (
                picks[:, None, first : first + group]
                + pointings * jnp.arange(2, dtype=jnp.int32)[:, None]
            ).reshape(-1)
            for first, group in zip(firsts, groups)
        ]
    )
    hot = (wanted[:, None] == jnp.arange(2 * pointings)[None, :]).astype(jnp.bfloat16)
    source = jnp.arange(local_time, dtype=jnp.int32)
    place = (source % inner) * LANES + source // inner
    perm = (place[:, None] == source[None, :]).astype(jnp.bfloat16)

    def form(groups, signal, rim):
        with_rim = rim is not None
        pieces = [(devices, local_subbands, inner, 2 * group, LANES) for group in groups]
        rim_size = (local_subbands, hot.shape[0], LANES)
        return pl.pallas_call(
            functools.partial(form_kernel, inner, groups, with_rim),
            grid=(local_subbands,),
            in_specs=[
                pl.BlockSpec(hot.shape, lambda s: (0, 0)),
                pl.BlockSpec(perm.shape, lambda s: (0, 0)),
                pl.BlockSpec((1, 2, pointings, inputs), lambda s: (s, 0, 0, 0)),
                pl.BlockSpec((1, 2 * inputs, local_time), lambda s: (s, 0, 0)),
            ]
            + [pl.BlockSpec((1, 2 * inputs, LANES), lambda s: (s, 0, 0))] * with_rim,
            out_specs=[pl.BlockSpec((1,) + rim_size[1:], lambda s: (s, 0, 0))] * with_rim
            + [
                pl.BlockSpec((size[0], 1) + size[2:], lambda s: (0, s, 0, 0, 0))
                for size in pieces
            ],
            out_shape=[jax.ShapeDtypeStruct(rim_size, jnp.bfloat16)] * with_rim
            + [jax.ShapeDtypeStruct(size, jnp.bfloat16) for size in pieces],
            compiler_params=pltpu.CompilerParams(vmem_limit_bytes=VMEM),
            cost_estimate=pl.CostEstimate(
                flops=12_000_000_000, bytes_accessed=20_000_000, transcendentals=0
            ),
            name="form",
        )(hot, perm, pointing_table, signal, *([rim] if with_rim else []))

    edge, opening = form(groups[:1], signal, rim)
    pieces = [opening]
    if len(groups) > 1:
        later, _ = lax.optimization_barrier((signal, opening))
        pieces += form(groups[1:], later, None)

    mat = synthesis_matrix(filter_taps, inner, reach)

    edge = edge[:, :, :rim_len]
    edge = jnp.concatenate(
        [
            edge[:, 2 * devices * start : 2 * devices * (start + group)].reshape(
                local_subbands, devices, 2 * group * rim_len
            )
            for start, group in zip(starts, groups)
        ],
        axis=2,
    )
    edge = edge.swapaxes(0, 1).reshape(devices, -1)
    edge_size = edge.shape[1]
    planes = -(-edge_size // (2 * groups[0] * LANES))
    edge = jnp.pad(edge, ((0, 0), (0, planes * 2 * groups[0] * LANES - edge_size)))
    edge = edge.reshape(devices, planes, 2 * groups[0], LANES)
    pieces = [
        piece.reshape(devices, local_subbands * inner, 2 * group, LANES)
        for piece, group in zip(pieces, groups)
    ]
    pieces[0] = jnp.concatenate([pieces[0], edge], axis=1)
    got = [lax.all_to_all(p, "sub", split_axis=0, concat_axis=0, tiled=True) for p in pieces]
    edge = got[0][:, local_subbands * inner :].reshape(devices, -1)[:, :edge_size]
    edge = jnp.take(edge.reshape(slots, -1), subband_order, axis=0)
    live_mask = jnp.arange(slots, dtype=jnp.int32) < live_subbands[0]
    edge = jnp.where(live_mask[:, None], edge.astype(jnp.float32), 0.0)

    def edge_of(start, group):
        part = edge[:, 2 * start * rim_len : 2 * (start + group) * rim_len]
        part = part.reshape(bands, chan, 2, group, reach - 1, inner)
        return part.transpose(0, 3, 2, 4, 5, 1).reshape(
            bands, group, 2, reach - 1, inner * chan
        )

    result = None
    for first, start, group, z in zip(firsts, starts, groups, got):
        operands = [subband_order, live_subbands, z, edge_of(start, group), mat]
        in_specs = [
            pl.BlockSpec(memory_space=pl.ANY),
            pl.BlockSpec((1, group, 2, reach - 1, LANES), lambda g, *_: (g, 0, 0, 0, 0)),
            pl.BlockSpec(mat.shape, lambda g, *_: (0, 0)),
        ]
        alias = {}
        if result is not None:
            operands.append(result)
            in_specs.append(pl.BlockSpec(memory_space=pl.ANY))
            alias = {5: 0}
        result = pl.pallas_call(
            functools.partial(synth_kernel, inner, chan, group, reach, local_subbands),
            grid_spec=pltpu.PrefetchScalarGridSpec(
                num_scalar_prefetch=2,
                grid=(bands,),
                in_specs=in_specs,
                out_specs=pl.BlockSpec(
                    (group, 1, 2, local_time * chan), functools.partial(lambda h, g, *_: (h, g, 0, 0), first // group)
                ),
                scratch_shapes=[
                    pltpu.VMEM((2, chan, inner, 2 * group, LANES), jnp.bfloat16),
                    pltpu.VMEM((inner, chan * 2 * group, LANES), jnp.float32),
                    pltpu.VMEM((2, 8 + LANES, LANES), jnp.float32),
                    pltpu.VMEM((group * LANES, mat.shape[0]), jnp.bfloat16),
                    pltpu.VMEM((2, 2 * LANES, LANES), jnp.float32),
                    pltpu.SemaphoreType.DMA((2,)),
                ],
            ),
            out_shape=jax.ShapeDtypeStruct((beam_part, bands, 2, local_time * chan), jnp.bfloat16),
            input_output_aliases=alias,
            compiler_params=pltpu.CompilerParams(vmem_limit_bytes=VMEM),
            cost_estimate=pl.CostEstimate(
                flops=10_000_000_000, bytes_accessed=13_000_000, transcendentals=0
            ),
            name="synth",
        )(*operands)

    return result

MESH = pl.DeviceIdType.MESH


def drain(ref, sem):
    pltpu.make_async_copy(ref, ref, sem).wait()


def relay_kernel(
    n,
    chan,
    order_ref,
    live_ref,
    pick_ref,
    table_ref,
    taps_ref,
    trig_ref,
    volt_ref,
    out_ref,
    z,
    own_out,
    far_out,
    volts,
    far_volts,
    chosen,
    far_chosen,
    own_w,
    far_w,
    lhs,
    stage,
    wide,
    select,
    steps,
    mat,
    made,
    ready,
    tail,
    tail_sent,
    rim,
    head,
    joint,
    redo,
    mended,
    z_sem,
    own_sem,
    far_sem,
    in_sem,
    volt_send,
    volt_recv,
    w_send,
    w_recv,
    fwd_send,
    fwd_recv,
    rim_sem,
    out_sem,
    mend_sem,
):
    f32, bf16 = jnp.float32, jnp.bfloat16
    half, quarter = n // 2, n // 4
    chunks, slots_here, inputs2, _ = volts.shape
    pair = z.shape[2]
    group = pair // 2
    bands = ready.shape[1]
    inner = LANES // chan
    spans = mat.shape[0] // pair_of(chan)
    halo = spans - inner
    blocks = LANES // inner
    ring = far_out.shape[0]
    together = wide.shape[0]
    pitch = wide.shape[1] // chan
    parts = volt_recv.shape[2]
    batch = slots_here // parts
    unroll = math.gcd(batch, 6)

    me, tm = lax.axis_index("sub"), lax.axis_index("tm")
    side, pos = lax.div(me, half), lax.rem(me, half)
    rank, lane = lax.div(pos, quarter), lax.rem(me, quarter)
    other = 1 - side
    is_gate = rank == 1 - side
    near = side
    gate = other * half + side * quarter + lane
    share = slots_here // 2
    mine = pl.ds(tm * share, share)
    theirs = pl.ds((1 - tm) * share, share)

    def chunk_at(step):
        return lax.rem(step + chunks - 1, chunks)

    def source_of(rank_from):
        return other * half + rank_from * quarter + lane

    def load(c):
        return pltpu.make_async_copy(
            volt_ref.at[:, :, pl.ds(pl.multiple_of(c * LANES, LANES), LANES)],
            volts.at[c],
            in_sem.at[c],
        )

    def send_volts(c):
        for part in range(parts):
            some = pl.ds(part * batch, batch)
            pltpu.make_async_remote_copy(
                src_ref=volts.at[c, some],
                dst_ref=far_volts.at[c, rank, some],
                send_sem=volt_send.at[c],
                recv_sem=volt_recv.at[c, rank, part],
                device_id=(gate, tm),
                device_id_type=MESH,
            ).start()

    def send_all(sent, src, c, sems, first, count):
        def to(j, carry):
            there = lax.rem(pos + 1 + j, half)
            pltpu.make_async_remote_copy(
                src_ref=sent.at[there, pl.ds(first, count)],
                dst_ref=z.at[c, pl.ds(src * slots_here + first, count)],
                send_sem=sems.at[there],
                recv_sem=z_sem.at[c, src],
                device_id=(side * half + there, tm),
                device_id_type=MESH,
            ).start()
            return carry

        lax.fori_loop(0, half - 1, to, 0)

    def wait_all(sent, sems):
        def one(j, carry):
            there = lax.rem(pos + 1 + j, half)
            drain(sent.at[there], sems.at[there])
            return carry

        lax.fori_loop(0, half - 1, one, 0)

    def form(weights, signal, sent, src, c, first, count):
        def one(j, carry):
            s = first + j
            formed = jnp.dot(
                weights[s][:, :inputs2], signal[s], preferred_element_type=f32
            ).astype(bf16)
            for d in range(half):
                sent[d, s] = formed[d * pair : (d + 1) * pair]
            return carry

        lax.fori_loop(0, count, one, 0, unroll=unroll)

    def keep(sent, src, c):
        def one(s, carry):
            z[c, src * slots_here + s] = sent[pos, s]
            return carry

        lax.fori_loop(0, slots_here, one, 0, unroll=unroll)

    def prepare(picked, weights, at):
        w = picked.astype(f32)
        real, imag = w[: inputs2 // 2], w[inputs2 // 2 :]
        rest = jnp.zeros((weights.shape[2] - inputs2, LANES), f32)
        upper = jnp.concatenate([real, -imag, rest], axis=0).T.astype(bf16)
        lower = jnp.concatenate([imag, real, rest], axis=0).T.astype(bf16)
        for d in range(half):
            rows = slice(d * group, (d + 1) * group)
            weights[at, d * pair : d * pair + group] = upper[rows]
            weights[at, d * pair + group : (d + 1) * pair] = lower[rows]

    load(chunk_at(0)).start()

    def send_later(step, carry):
        load(chunk_at(step)).wait()
        send_volts(chunk_at(step))
        return carry

    send_later(0, 0)
    for step in range(1, chunks):
        load(chunk_at(step)).start()

    pointings = table_ref.shape[2]
    hot = (
        lax.broadcasted_iota(jnp.int32, (pointings, 2 * LANES), 0) == pick_ref[...]
    ).astype(bf16)

    def choose(s, carry):
        picked = jnp.dot(table_ref[s], hot, preferred_element_type=f32).astype(bf16)
        chosen[0, s] = picked[:, :LANES]
        chosen[1, s] = picked[:, LANES:]
        return carry

    lax.fori_loop(0, slots_here, choose, 0)

    def send_weights():
        pltpu.make_async_remote_copy(
            src_ref=chosen.at[other, mine],
            dst_ref=far_chosen.at[rank, mine],
            send_sem=w_send,
            recv_sem=w_recv.at[rank],
            device_id=(gate, tm),
            device_id_type=MESH,
        ).start()

    send_weights()
    lax.fori_loop(1, chunks, send_later, 0)

    def prepare_own(s, carry):
        prepare(chosen[side, s], own_w, s)
        return carry

    lax.fori_loop(0, slots_here, prepare_own, 0)

    tap_count = taps_ref.shape[0]
    repeat = lax.broadcasted_iota(jnp.int32, (chan, LANES), 0) == lax.rem(
        lax.broadcasted_iota(jnp.int32, (chan, LANES), 1), chan
    )
    taps = jnp.dot(
        taps_ref[...],
        repeat.astype(f32),
        precision=lax.Precision.HIGHEST,
        preferred_element_type=f32,
    )
    tap_at = lax.broadcasted_iota(jnp.int32, (tap_count, LANES), 0)
    time_at = lax.div(lax.broadcasted_iota(jnp.int32, (tap_count, LANES), 1), chan)
    for v in range(spans):
        row = jnp.sum(
            jnp.where(time_at - tap_at == v - halo, taps, 0.0), axis=0, keepdims=True
        )
        mat[v * 2 * chan : (v + 1) * 2 * chan] = (
            jnp.concatenate([row, row], axis=1) * trig_ref[...]
        ).astype(bf16)
    select_row = lax.broadcasted_iota(jnp.int32, (LANES, LANES), 0)
    phases = LANES // (2 * chan)
    select_time = lax.rem(select_row, LANES // phases) * phases + lax.div(
        select_row, LANES // phases
    )
    select[...] = (
        lax.broadcasted_iota(jnp.int32, (LANES, LANES), 1) == select_time
    ).astype(bf16)
    tail[...] = jnp.zeros_like(tail)

    def foreign_weights(k):
        forward = pltpu.make_async_remote_copy(
            src_ref=far_chosen.at[k, mine],
            dst_ref=far_chosen.at[k, mine],
            send_sem=fwd_send.at[k],
            recv_sem=fwd_recv.at[k],
            device_id=(me, 1 - tm),
            device_id_type=MESH,
        )
        drain(far_chosen.at[k, mine], w_recv.at[k])
        forward.start()
        drain(far_chosen.at[k, theirs], fwd_recv.at[k])

        def one(s, carry):
            prepare(far_chosen[k, s], far_w.at[k], s)
            return carry

        lax.fori_loop(0, slots_here, one, 0)
        drain(far_chosen.at[k, mine], fwd_send.at[k])

    def foreign(k, i, turn):
        c = chunk_at(i)
        slot = lax.rem(turn, ring)

        @pl.when(i == 0)
        def _():
            foreign_weights(k)

        @pl.when(turn >= ring)
        def _():
            wait_all(far_out.at[slot], far_sem.at[slot])

        src = source_of(k)

        def one(part, carry):
            first = part * batch
            drain(far_volts.at[c, k, pl.ds(first, batch)], volt_recv.at[c, k, part])
            form(far_w.at[k], far_volts.at[c, k], far_out.at[slot], src, c, first, batch)
            send_all(far_out.at[slot], src, c, far_sem.at[slot], first, batch)
            return carry

        lax.fori_loop(0, parts, one, 0)
        keep(far_out.at[slot], src, c)

    width = 2 * chan
    fold = LANES // width
    lanes_at = lax.broadcasted_iota(jnp.int32, (LANES // fold, LANES), 1)

    def swap(one, two, size):
        low = lax.rem(lanes_at, 2 * size) < size
        return (
            jnp.where(low, one, pltpu.roll(two, size, 1)),
            jnp.where(low, pltpu.roll(one, LANES - size, 1), two),
        )

    def exchange(parts):
        first, third = swap(parts[0], parts[2], 2 * width)
        second, fourth = swap(parts[1], parts[3], 2 * width)
        return swap(first, second, width) + swap(third, fourth, width)

    def synthesise(i):
        c = chunk_at(i - 1)

        def one(src, carry):
            local = (src == me) | (
                is_gate & (lax.div(src, half) == other) & (lax.rem(src, quarter) == lane)
            )

            @pl.when(jnp.logical_not(local))
            def _():
                drain(z.at[c, pl.ds(src * slots_here, slots_here)], z_sem.at[c, src])

            return carry

        lax.fori_loop(0, n, one, 0)

        def copy(s, carry):
            stage[s] = z[c, s]
            return carry

        lax.fori_loop(0, stage.shape[0], copy, 0, unroll=4)

        def gather(g, at_once):
            for k in range(chan):
                alive = g * chan + k < live_ref[0]
                block = stage[order_ref[g * chan + k]].astype(f32)
                wide[at_once, k * pitch : k * pitch + pair] = jnp.where(alive, block, 0.0)

            for q in range(group // fold):
                rows = [
                    wide[at_once, pl.ds(p * group + q * fold + b, chan, stride=pitch), :]
                    for b in range(fold)
                    for p in range(2)
                ]
                turned = lax.dot_general(
                    select[...],
                    jnp.concatenate(rows, axis=0).astype(bf16),
                    (((1,), (1,)), ((), ())),
                    preferred_element_type=f32,
                )
                size = LANES // fold
                split = [turned[w * size : (w + 1) * size] for w in range(fold)]
                for b, block in enumerate(exchange(split)):
                    beam = q * fold + b
                    at = g * group + beam
                    steps[at_once, beam, :8] = tail[at]
                    steps[at_once, beam, 8:] = block
                    tail[at] = block[LANES // fold - 8 :]
                    head[lax.min(i - 1, 1), at] = block[:8]
                    for e in range(spans // fold):
                        lhs[e, beam, pl.ds(pl.multiple_of(g * blocks, blocks), blocks)] = steps[
                            at_once, beam, pl.ds(8 - halo // fold + e, blocks, stride=inner // fold), :
                        ].astype(bf16)

        def several(j, carry):
            for at_once in range(together):
                gather(j * together + at_once, at_once)
            return carry

        lax.fori_loop(0, bands // together, several, 0)

        out_copy = pltpu.make_async_copy(
            ready,
            out_ref.at[:, :, pl.ds(pl.multiple_of(c * 2 * blocks, 2 * blocks), 2 * blocks)],
            out_sem,
        )

        @pl.when(i > 1)
        def _():
            drain(ready, out_sem)

        def emit(b, carry):
            rows = bands * blocks
            terms = [
                lhs[e, pl.ds(b * fold, fold)].reshape(fold * rows, LANES)
                for e in range(spans // fold)
            ]
            out = jnp.dot(
                jnp.concatenate(terms, axis=1), mat[...], preferred_element_type=f32
            )
            made[pl.ds(0, fold * rows, stride=2), :] = out[:, :LANES]
            made[pl.ds(1, fold * rows, stride=2), :] = out[:, LANES:]
            for j in range(fold):
                for g in range(bands):
                    at = (j * bands + g) * 2 * blocks
                    ready[b * fold + j, g] = made[at : at + 2 * blocks].astype(bf16)
            return carry

        lax.fori_loop(0, group // fold, emit, 0)
        out_copy.start()

    def patch():
        rows = halo // inner + 2
        opening = bands * rows

        def restack(b, carry):
            for g in range(bands):
                at = g * group + b
                joint[g, :8] = tail[at]
                joint[g, 8:] = head[0, at]
                for e in range(spans // fold):
                    redo[e, b, g * rows : (g + 1) * rows] = joint[
                        g, pl.ds(8 - halo // fold + e, rows, stride=inner // fold), :
                    ]
            return carry

        lax.fori_loop(0, group, restack, 0)
        terms = [
            redo[e].reshape(group * opening, LANES).astype(bf16) for e in range(spans // fold)
        ]
        out = jnp.dot(jnp.concatenate(terms, axis=1), mat[...], preferred_element_type=f32)
        made[pl.ds(0, group * opening, stride=2), :] = out[:, :LANES]
        made[pl.ds(1, group * opening, stride=2), :] = out[:, LANES:]

        def place(b, carry):
            for g in range(bands):
                at = pl.multiple_of(b * opening * 2 + g * rows * 2, rows * 2)
                mended[b, g] = made[pl.ds(at, rows * 2)].astype(bf16)
            return carry

        lax.fori_loop(0, group, place, 0)
        c = chunk_at(0)
        start = pl.multiple_of(c * 2 * blocks, 2 * blocks)
        copy = pltpu.make_async_copy(
            mended, out_ref.at[:, :, pl.ds(start, rows * 2)], mend_sem
        )
        copy.start()
        copy.wait()

    def pass_tail():
        return pltpu.make_async_remote_copy(
            src_ref=tail_sent,
            dst_ref=rim,
            send_sem=rim_sem.at[0],
            recv_sem=rim_sem.at[1],
            device_id=(me, 1),
            device_id_type=MESH,
        )

    def own(i, carry):
        c = chunk_at(i)
        form(own_w, volts.at[c], own_out.at[c], me, c, 0, slots_here)
        send_all(own_out.at[c], me, c, own_sem.at[c], 0, slots_here)
        keep(own_out.at[c], me, c)
        return carry

    ahead, prompt = 3, chunks
    lax.fori_loop(0, ahead, own, 0)

    def early(i, carry):
        later = i + ahead

        @pl.when((later < prompt) | (jnp.logical_not(is_gate) & (later < chunks)))
        def _():
            own(later, 0)

        @pl.when(is_gate)
        def _():
            foreign(1 - near, i, i)

        return carry

    lax.fori_loop(0, chunks, early, 0)

    def step(i, carry):
        @pl.when(is_gate & (i < chunks))
        def _():
            foreign(near, i, chunks + i)

        @pl.when(is_gate & (i + prompt < chunks))
        def _():
            own(i + prompt, 0)

        @pl.when((i == 2) & (tm == 0))
        def _():
            tail[...] = jnp.zeros_like(tail)

        @pl.when((i == 2) & (tm == 1))
        def _():
            drain(rim, rim_sem.at[1])

            def one(j, carry):
                tail[2 * j] = rim[j, :8].astype(f32)
                tail[2 * j + 1] = rim[j, 8:].astype(f32)
                return carry

            lax.fori_loop(0, rim.shape[0], one, 0)

        @pl.when(i >= 1)
        def _():
            synthesise(i)

        @pl.when((i == 1) & (tm == 0))
        def _():
            def one(j, carry):
                pair_at = jnp.concatenate([tail[2 * j], tail[2 * j + 1]], axis=0)
                tail_sent[j] = pair_at.astype(bf16)
                return carry

            lax.fori_loop(0, rim.shape[0], one, 0)
            pass_tail().start()

        return carry

    lax.fori_loop(0, chunks + 1, step, 0)
    patch()

    drain(ready, out_sem)
    drain(chosen.at[other, mine], w_send)

    @pl.when(tm == 0)
    def _():
        drain(tail_sent, rim_sem.at[0])

    def finish(c, carry):
        drain(volts.at[c], volt_send.at[c])
        wait_all(own_out.at[c], own_sem.at[c])
        return carry

    lax.fori_loop(0, chunks, finish, 0)

    @pl.when(is_gate)
    def _():
        def one(slot, carry):
            wait_all(far_out.at[slot], far_sem.at[slot])
            return carry

        lax.fori_loop(0, ring, one, 0)


def hand_over_kernel(in_ref, out_ref, held, in_sem, out_sem):
    count = held.shape[0]
    reads = [pltpu.make_async_copy(in_ref.at[b], held.at[b], in_sem.at[b]) for b in range(count)]
    writes = [
        pltpu.make_async_copy(held.at[b], out_ref.at[b], out_sem.at[b]) for b in range(count)
    ]
    for read in reads:
        read.start()
    for read, write in zip(reads, writes):
        read.wait()
        write.start()
    for write in writes:
        write.wait()


def pair_of(chan):
    return 2 * chan


def relay_plan(voltages, pointing_table, beam_pointing, subband_order, live_subbands, filter_taps):
    local, _, inputs, local_time = voltages.shape
    pointings = pointing_table.shape[2]
    beams = beam_pointing.shape[0]
    slots = subband_order.shape[0]
    tap_count, chan = filter_taps.shape
    n = lax.axis_size("sub")
    half = n // 2
    group = beams // n
    pair = 2 * group
    inner = LANES // chan
    spans = inner * (1 + -(-(tap_count - 1) // inner))
    halo = spans - inner
    chunks = local_time // LANES
    bands = slots // chan
    blocks = LANES // inner
    fold = LANES // (2 * chan)
    bf16, f32 = jnp.bfloat16, jnp.float32
    ring = 4
    together = math.gcd(bands, 2)

    at = np.arange(chan)
    phase = (np.outer(at, at) % chan).astype(np.float32) * np.float32(2.0 * math.pi / chan)
    cosine, sine = (
        np.asarray(f(phase), jnp.bfloat16).astype(np.float32) for f in (np.cos, np.sin)
    )
    trig = np.stack([np.stack([cosine, -sine], 1), np.stack([sine, cosine], 1)])
    trig = trig.transpose(2, 3, 0, 1)[:, :, :, None, :]
    trig = np.broadcast_to(trig, (2, chan, 2, inner, chan))
    trig = jnp.asarray(trig.reshape(2 * chan, 2 * LANES))
    signal = voltages.reshape(local, 2 * inputs, local_time)
    table = pointing_table.transpose(0, 1, 3, 2).reshape(local, 2 * inputs, pointings)
    lanes_in = 2 * LANES

    vmem = pl.BlockSpec(memory_space=pltpu.VMEM)
    smem = pl.BlockSpec(memory_space=pltpu.SMEM)
    anywhere = pl.BlockSpec(memory_space=pl.ANY)
    dma = pltpu.SemaphoreType.DMA
    out = pl.pallas_call(
        functools.partial(relay_kernel, n, chan),
        in_specs=[smem, smem, vmem, vmem, vmem, vmem, anywhere],
        out_specs=anywhere,
        out_shape=jax.ShapeDtypeStruct((group, bands, 2 * blocks * chunks, LANES), bf16),
        scratch_shapes=[
            pltpu.VMEM((chunks, slots, pair, LANES), bf16),
            pltpu.VMEM((chunks, half, local, pair, LANES), bf16),
            pltpu.VMEM((ring, half, local, pair, LANES), bf16),
            pltpu.VMEM((chunks, local, 2 * inputs, LANES), bf16),
            pltpu.VMEM((chunks, 2, local, 2 * inputs, LANES), bf16),
            pltpu.VMEM((2, local, 2 * inputs, LANES), bf16),
            pltpu.VMEM((2, local, 2 * inputs, LANES), bf16),
            pltpu.VMEM((local, half * pair, lanes_in), bf16),
            pltpu.VMEM((2, local, half * pair, lanes_in), bf16),
            pltpu.VMEM((spans // fold, group, bands * blocks, LANES), bf16),
            pltpu.VMEM((slots, pair, LANES), bf16),
            pltpu.VMEM((together, chan * (pair + 1), LANES), f32),
            pltpu.VMEM((LANES, LANES), bf16),
            pltpu.VMEM((together, group, 8 + LANES // fold, LANES), f32),
            pltpu.VMEM((spans * 2 * chan, 2 * LANES), bf16),
            pltpu.VMEM((fold * bands * blocks * 2, LANES), f32),
            pltpu.VMEM((group, bands, 2 * blocks, LANES), bf16),
            pltpu.VMEM((bands * group, 8, LANES), f32),
            pltpu.VMEM((bands * group // 2, 16, LANES), bf16),
            pltpu.VMEM((bands * group // 2, 16, LANES), bf16),
            pltpu.VMEM((2, bands * group, 8, LANES), f32),
            pltpu.VMEM((bands, 16, LANES), f32),
            pltpu.VMEM((spans // fold, group, bands * (halo // inner + 2), LANES), f32),
            pltpu.VMEM((group, bands, 2 * (halo // inner + 2), LANES), bf16),
            dma((chunks, n)),
            dma((chunks, half)),
            dma((ring, half)),
            dma((chunks,)),
            dma((chunks,)),
            dma((chunks, 2, 2)),
            dma,
            dma((2,)),
            dma((2,)),
            dma((2,)),
            dma((2,)),
            dma,
            dma,
        ],
        compiler_params=pltpu.CompilerParams(
            vmem_limit_bytes=66_000_000, has_side_effects=True
        ),
        cost_estimate=pl.CostEstimate(
            flops=20_000_000_000, bytes_accessed=20_000_000, transcendentals=0
        ),
        name="relay",
    )(
        subband_order,
        live_subbands,
        beam_pointing.reshape(1, beams),
        table,
        filter_taps,
        trig,
        signal,
    )
    out = pl.pallas_call(
        hand_over_kernel,
        in_specs=[anywhere],
        out_specs=anywhere,
        out_shape=jax.ShapeDtypeStruct(out.shape, bf16),
        scratch_shapes=[pltpu.VMEM(out.shape, bf16), dma((group,)), dma((group,))],
        compiler_params=pltpu.CompilerParams(vmem_limit_bytes=VMEM),
        name="hand_over",
    )(out)
    out = out.reshape(group, bands, blocks * chunks, 2, LANES).transpose(0, 1, 3, 2, 4)
    return out.reshape(group, bands, 2, local_time * chan)


def on_device(voltages, pointing_table, beam_pointing, subband_order, live_subbands, filter_taps):
    local, _, inputs, local_time = voltages.shape
    beams = beam_pointing.shape[0]
    tap_count, chan = filter_taps.shape
    n = lax.axis_size("sub")
    fits = (
        lax.axis_size("tm") == 2
        and n % 4 == 0
        and beams == 2 * LANES
        and beams // n % 8 == 0
        and local % 2 == 0
        and local_time % LANES == 0
        and local_time >= 4 * LANES
        and chan * 8 == LANES
        and tap_count <= chan + 1
    )
    plan = relay_plan if fits else direct_plan
    return plan(
        voltages, pointing_table, beam_pointing, subband_order, live_subbands, filter_taps
    )


def solution(mesh):
    in_specs = (P("sub", None, None, "tm"), P("sub", None, None, None), P(), P(), P(), P())
    out_specs = P("sub", None, None, "tm")
    return jax.shard_map(
        on_device, mesh=mesh, in_specs=in_specs, out_specs=out_specs, check_vma=False
    )
```

```python
import functools
import math

import jax
import jax.numpy as jnp
import numpy as np
from jax import lax
from jax.experimental import pallas as pl
from jax.experimental.pallas import tpu as pltpu
from jax.sharding import PartitionSpec as P

LANES = 128
VMEM = 60 * 1024 * 1024


def inverse_table(channel_count):
    channel_index = jnp.arange(channel_count, dtype=jnp.int32)
    phase = (jnp.outer(channel_index, channel_index) % channel_count).astype(jnp.float32) * (
        2.0 * math.pi / channel_count
    )
    cosine = jnp.cos(phase).astype(jnp.bfloat16)
    sine_table = jnp.sin(phase).astype(jnp.bfloat16)
    upper_rows = jnp.stack([cosine, -sine_table], axis=1)
    lower_rows = jnp.stack([sine_table, cosine], axis=1)
    return jnp.stack([upper_rows, lower_rows], axis=0)


def synthesis_matrix(filter_taps, inner, reach):
    tap_count, chan = filter_taps.shape
    table = inverse_table(chan).astype(jnp.float32)
    delta = jnp.arange(reach)[:, None, None]
    tl_in = jnp.arange(inner)[None, :, None]
    tl_out = jnp.arange(inner)[None, None, :]
    tap = inner * delta + tl_out - tl_in
    inside = (tap >= 0) & (tap < tap_count)
    taps = jnp.where(inside[..., None], filter_taps[jnp.clip(tap, 0, tap_count - 1)], 0.0)
    full = (
        taps[:, None, :, None, None, :, :]
        * table.transpose(2, 3, 0, 1)[None, :, None, :, :, None, :]
    )
    return full.reshape(reach * 2 * inner * chan, 2 * inner * chan).astype(jnp.bfloat16)


def form_kernel(inner, groups, with_rim, hot_ref, perm_ref, table_ref, volt_ref, *rest):
    chunks = rest[-len(groups) :]
    f32, bf16 = jnp.float32, jnp.bfloat16
    real, imag = table_ref[0, 0], table_ref[0, 1]
    both = jnp.concatenate(
        [
            jnp.concatenate([real, -imag], axis=1),
            jnp.concatenate([imag, real], axis=1),
        ],
        axis=0,
    )
    weights = jnp.dot(hot_ref[...], both, preferred_element_type=f32).astype(bf16)
    if with_rim:
        rim_ref, rim_out = rest[0], rest[1]
        rim_out[0] = jnp.dot(weights, rim_ref[0], preferred_element_type=f32).astype(bf16)
    signal = jnp.dot(volt_ref[0], perm_ref[...], preferred_element_type=f32).astype(bf16)
    start = 0 if with_rim else hot_ref.shape[0] - 2 * sum(groups) * chunks[0].shape[0]
    for group, out in zip(groups, chunks):
        rows = 2 * group * out.shape[0]
        formed = jnp.dot(
            weights[start : start + rows], signal, preferred_element_type=f32
        ).astype(bf16)
        start += rows
        for d in range(out.shape[0]):
            for tl in range(inner):
                out[d, 0, tl] = formed[
                    2 * d * group : 2 * (d + 1) * group, tl * LANES : (tl + 1) * LANES
                ]


def synth_kernel(
    inner, chan, group, reach, local, order_ref, live_ref, z_ref, rim_ref, mat_ref, *rest
):
    out_ref, held, wide, line, stacked, made, sems = rest[-7:]
    g = pl.program_id(0)
    count = pl.num_programs(0)
    f32, bf16 = jnp.float32, jnp.bfloat16

    def fetch(step, slot):
        named = [order_ref[step * chan + c] for c in range(chan)]
        return [
            pltpu.make_async_copy(
                z_ref.at[lax.div(at, local), pl.ds(lax.rem(at, local) * inner, inner)],
                held.at[slot, c],
                sems.at[slot],
            )
            for c, at in enumerate(named)
        ]

    slot = lax.rem(g, 2)

    @pl.when(g == 0)
    def _():
        for copy in fetch(0, 0):
            copy.start()

    @pl.when(g + 1 < count)
    def _():
        for copy in fetch(g + 1, 1 - slot):
            copy.start()

    for copy in fetch(g, slot):
        copy.wait()

    pair = 2 * group
    for c in range(chan):
        alive = g * chan + c < live_ref[0]
        for tl in range(inner):
            block = held[slot, c, tl].astype(f32)
            wide[tl, c * pair : (c + 1) * pair, :] = jnp.where(alive, block, 0.0)

    width = inner * chan

    def turn(b, carry):
        base = pl.multiple_of(b * LANES, LANES)
        for p in range(2):
            rows = [
                wide[tl, pl.ds(p * group + b, chan, stride=pair), :] for tl in range(inner)
            ]
            line[p, 8 : 8 + LANES, :] = jnp.concatenate(rows, axis=0).T
            line[p, 8 - (reach - 1) : 8, :] = rim_ref[0, b, p]
            for delta in range(reach):
                at = (2 * delta + p) * width
                stacked[pl.ds(base, LANES), at : at + width] = line[
                    p, 8 - delta : 8 - delta + LANES, :
                ].astype(bf16)
        return carry

    lax.fori_loop(0, group, turn, 0, unroll=2)

    def emit(b, carry):
        base = pl.multiple_of(b * 2 * LANES, 2 * LANES)
        out = jnp.dot(
            stacked[pl.ds(base, 2 * LANES), :], mat_ref[...], preferred_element_type=f32
        )
        for i in range(2):
            for q in range(2):
                made[i, q * LANES : (q + 1) * LANES, :] = out[
                    i * LANES : (i + 1) * LANES, q * width : (q + 1) * width
                ]
        for i in range(2):
            for tb in range(LANES):
                both = made[i, pl.ds(tb, 2, stride=LANES), :].astype(bf16)
                out_ref[2 * b + i, 0, :, tb * LANES : (tb + 1) * LANES] = both
        return carry

    lax.fori_loop(0, group // 2, emit, 0)


def direct_plan(voltages, pointing_table, beam_pointing, subband_order, live_subbands, filter_taps):
    local_subbands, _, inputs, local_time = voltages.shape
    pointings = pointing_table.shape[2]
    beam_count = beam_pointing.shape[0]
    slots = subband_order.shape[0]
    tap_count, chan = filter_taps.shape
    inner = LANES // chan
    assert local_time == inner * LANES
    reach = 1 + -(-(tap_count - 1) // inner)
    rim_len = (reach - 1) * inner
    devices = lax.axis_size("sub")
    beam_part = beam_count // devices
    quarter = beam_part // 4
    if beam_part % 8 == 0:
        groups, firsts = [quarter, 2 * quarter, quarter], [0, 2 * quarter, quarter]
    else:
        groups, firsts = [beam_part], [0]
    starts = [sum(groups[:h]) for h in range(len(groups))]
    bands = slots // chan

    signal = voltages.reshape(local_subbands, 2 * inputs, local_time)
    times = range(lax.axis_size("tm"))
    route = [(i - 1, i) for i in times if i > 0]
    rim = lax.ppermute(signal[:, :, local_time - rim_len :], "tm", route)
    rim = jnp.pad(rim, ((0, 0), (0, 0), (0, LANES - rim_len)))

    picks = beam_pointing.reshape(devices, beam_part)
    wanted = jnp.concatenate(
        [
            (
                picks[:, None, first : first + group]
                + pointings * jnp.arange(2, dtype=jnp.int32)[:, None]
            ).reshape(-1)
            for first, group in zip(firsts, groups)
        ]
    )
    hot = (wanted[:, None] == jnp.arange(2 * pointings)[None, :]).astype(jnp.bfloat16)
    source = jnp.arange(local_time, dtype=jnp.int32)
    place = (source % inner) * LANES + source // inner
    perm = (place[:, None] == source[None, :]).astype(jnp.bfloat16)

    def form(groups, signal, rim):
        with_rim = rim is not None
        pieces = [(devices, local_subbands, inner, 2 * group, LANES) for group in groups]
        rim_size = (local_subbands, hot.shape[0], LANES)
        return pl.pallas_call(
            functools.partial(form_kernel, inner, groups, with_rim),
            grid=(local_subbands,),
            in_specs=[
                pl.BlockSpec(hot.shape, lambda s: (0, 0)),
                pl.BlockSpec(perm.shape, lambda s: (0, 0)),
                pl.BlockSpec((1, 2, pointings, inputs), lambda s: (s, 0, 0, 0)),
                pl.BlockSpec((1, 2 * inputs, local_time), lambda s: (s, 0, 0)),
            ]
            + [pl.BlockSpec((1, 2 * inputs, LANES), lambda s: (s, 0, 0))] * with_rim,
            out_specs=[pl.BlockSpec((1,) + rim_size[1:], lambda s: (s, 0, 0))] * with_rim
            + [
                pl.BlockSpec((size[0], 1) + size[2:], lambda s: (0, s, 0, 0, 0))
                for size in pieces
            ],
            out_shape=[jax.ShapeDtypeStruct(rim_size, jnp.bfloat16)] * with_rim
            + [jax.ShapeDtypeStruct(size, jnp.bfloat16) for size in pieces],
            compiler_params=pltpu.CompilerParams(vmem_limit_bytes=VMEM),
            cost_estimate=pl.CostEstimate(
                flops=12_000_000_000, bytes_accessed=20_000_000, transcendentals=0
            ),
            name="form",
        )(hot, perm, pointing_table, signal, *([rim] if with_rim else []))

    edge, opening = form(groups[:1], signal, rim)
    pieces = [opening]
    if len(groups) > 1:
        later, _ = lax.optimization_barrier((signal, opening))
        pieces += form(groups[1:], later, None)

    mat = synthesis_matrix(filter_taps, inner, reach)

    edge = edge[:, :, :rim_len]
    edge = jnp.concatenate(
        [
            edge[:, 2 * devices * start : 2 * devices * (start + group)].reshape(
                local_subbands, devices, 2 * group * rim_len
            )
            for start, group in zip(starts, groups)
        ],
        axis=2,
    )
    edge = edge.swapaxes(0, 1).reshape(devices, -1)
    edge_size = edge.shape[1]
    planes = -(-edge_size // (2 * groups[0] * LANES))
    edge = jnp.pad(edge, ((0, 0), (0, planes * 2 * groups[0] * LANES - edge_size)))
    edge = edge.reshape(devices, planes, 2 * groups[0], LANES)
    pieces = [
        piece.reshape(devices, local_subbands * inner, 2 * group, LANES)
        for piece, group in zip(pieces, groups)
    ]
    pieces[0] = jnp.concatenate([pieces[0], edge], axis=1)
    got = [lax.all_to_all(p, "sub", split_axis=0, concat_axis=0, tiled=True) for p in pieces]
    edge = got[0][:, local_subbands * inner :].reshape(devices, -1)[:, :edge_size]
    edge = jnp.take(edge.reshape(slots, -1), subband_order, axis=0)
    live_mask = jnp.arange(slots, dtype=jnp.int32) < live_subbands[0]
    edge = jnp.where(live_mask[:, None], edge.astype(jnp.float32), 0.0)

    def edge_of(start, group):
        part = edge[:, 2 * start * rim_len : 2 * (start + group) * rim_len]
        part = part.reshape(bands, chan, 2, group, reach - 1, inner)
        return part.transpose(0, 3, 2, 4, 5, 1).reshape(
            bands, group, 2, reach - 1, inner * chan
        )

    result = None
    for first, start, group, z in zip(firsts, starts, groups, got):
        operands = [subband_order, live_subbands, z, edge_of(start, group), mat]
        in_specs = [
            pl.BlockSpec(memory_space=pl.ANY),
            pl.BlockSpec((1, group, 2, reach - 1, LANES), lambda g, *_: (g, 0, 0, 0, 0)),
            pl.BlockSpec(mat.shape, lambda g, *_: (0, 0)),
        ]
        alias = {}
        if result is not None:
            operands.append(result)
            in_specs.append(pl.BlockSpec(memory_space=pl.ANY))
            alias = {5: 0}
        result = pl.pallas_call(
            functools.partial(synth_kernel, inner, chan, group, reach, local_subbands),
            grid_spec=pltpu.PrefetchScalarGridSpec(
                num_scalar_prefetch=2,
                grid=(bands,),
                in_specs=in_specs,
                out_specs=pl.BlockSpec(
                    (group, 1, 2, local_time * chan), functools.partial(lambda h, g, *_: (h, g, 0, 0), first // group)
                ),
                scratch_shapes=[
                    pltpu.VMEM((2, chan, inner, 2 * group, LANES), jnp.bfloat16),
                    pltpu.VMEM((inner, chan * 2 * group, LANES), jnp.float32),
                    pltpu.VMEM((2, 8 + LANES, LANES), jnp.float32),
                    pltpu.VMEM((group * LANES, mat.shape[0]), jnp.bfloat16),
                    pltpu.VMEM((2, 2 * LANES, LANES), jnp.float32),
                    pltpu.SemaphoreType.DMA((2,)),
                ],
            ),
            out_shape=jax.ShapeDtypeStruct((beam_part, bands, 2, local_time * chan), jnp.bfloat16),
            input_output_aliases=alias,
            compiler_params=pltpu.CompilerParams(vmem_limit_bytes=VMEM),
            cost_estimate=pl.CostEstimate(
                flops=10_000_000_000, bytes_accessed=13_000_000, transcendentals=0
            ),
            name="synth",
        )(*operands)

    return result

MESH = pl.DeviceIdType.MESH


def drain(ref, sem):
    pltpu.make_async_copy(ref, ref, sem).wait()


def relay_kernel(
    n,
    chan,
    order_ref,
    live_ref,
    pick_ref,
    table_ref,
    taps_ref,
    trig_ref,
    volt_ref,
    out_ref,
    z,
    own_out,
    far_out,
    volts,
    far_volts,
    chosen,
    far_chosen,
    own_w,
    far_w,
    lhs,
    stage,
    wide,
    select,
    steps,
    mat,
    made,
    ready,
    tail,
    tail_sent,
    rim,
    head,
    joint,
    redo,
    mended,
    z_sem,
    own_sem,
    far_sem,
    in_sem,
    volt_send,
    volt_recv,
    w_send,
    w_recv,
    fwd_send,
    fwd_recv,
    rim_sem,
    out_sem,
    mend_sem,
):
    f32, bf16 = jnp.float32, jnp.bfloat16
    half, quarter = n // 2, n // 4
    chunks, slots_here, inputs2, _ = volts.shape
    pair = z.shape[2]
    group = pair // 2
    bands = ready.shape[1]
    inner = LANES // chan
    spans = mat.shape[0] // pair_of(chan)
    halo = spans - inner
    blocks = LANES // inner
    ring = far_out.shape[0]
    together = wide.shape[0]
    pitch = wide.shape[1] // chan
    parts = volt_recv.shape[2]
    batch = slots_here // parts
    unroll = math.gcd(batch, 6)

    me, tm = lax.axis_index("sub"), lax.axis_index("tm")
    side, pos = lax.div(me, half), lax.rem(me, half)
    rank, lane = lax.div(pos, quarter), lax.rem(me, quarter)
    other = 1 - side
    is_gate = rank == 1 - side
    near = side
    gate = other * half + side * quarter + lane
    share = slots_here // 2
    mine = pl.ds(tm * share, share)
    theirs = pl.ds((1 - tm) * share, share)

    def chunk_at(step):
        return lax.rem(step + chunks - 1, chunks)

    def source_of(rank_from):
        return other * half + rank_from * quarter + lane

    def load(c):
        return pltpu.make_async_copy(
            volt_ref.at[:, :, pl.ds(pl.multiple_of(c * LANES, LANES), LANES)],
            volts.at[c],
            in_sem.at[c],
        )

    def send_volts(c):
        for part in range(parts):
            some = pl.ds(part * batch, batch)
            pltpu.make_async_remote_copy(
                src_ref=volts.at[c, some],
                dst_ref=far_volts.at[c, rank, some],
                send_sem=volt_send.at[c],
                recv_sem=volt_recv.at[c, rank, part],
                device_id=(gate, tm),
                device_id_type=MESH,
            ).start()

    def send_all(sent, src, c, sems, first, count):
        def to(j, carry):
            there = lax.rem(pos + 1 + j, half)
            pltpu.make_async_remote_copy(
                src_ref=sent.at[there, pl.ds(first, count)],
                dst_ref=z.at[c, pl.ds(src * slots_here + first, count)],
                send_sem=sems.at[there],
                recv_sem=z_sem.at[c, src],
                device_id=(side * half + there, tm),
                device_id_type=MESH,
            ).start()
            return carry

        lax.fori_loop(0, half - 1, to, 0)

    def wait_all(sent, sems):
        def one(j, carry):
            there = lax.rem(pos + 1 + j, half)
            drain(sent.at[there], sems.at[there])
            return carry

        lax.fori_loop(0, half - 1, one, 0)

    def form(weights, signal, sent, src, c, first, count):
        def one(j, carry):
            s = first + j
            formed = jnp.dot(
                weights[s][:, :inputs2], signal[s], preferred_element_type=f32
            ).astype(bf16)
            for d in range(half):
                sent[d, s] = formed[d * pair : (d + 1) * pair]
            return carry

        lax.fori_loop(0, count, one, 0, unroll=unroll)

    def keep(sent, src, c):
        def one(s, carry):
            z[c, src * slots_here + s] = sent[pos, s]
            return carry

        lax.fori_loop(0, slots_here, one, 0, unroll=unroll)

    def prepare(picked, weights, at):
        w = picked.astype(f32)
        real, imag = w[: inputs2 // 2], w[inputs2 // 2 :]
        rest = jnp.zeros((weights.shape[2] - inputs2, LANES), f32)
        upper = jnp.concatenate([real, -imag, rest], axis=0).T.astype(bf16)
        lower = jnp.concatenate([imag, real, rest], axis=0).T.astype(bf16)
        for d in range(half):
            rows = slice(d * group, (d + 1) * group)
            weights[at, d * pair : d * pair + group] = upper[rows]
            weights[at, d * pair + group : (d + 1) * pair] = lower[rows]

    load(chunk_at(0)).start()

    def send_later(step, carry):
        load(chunk_at(step)).wait()
        send_volts(chunk_at(step))
        return carry

    send_later(0, 0)
    for step in range(1, chunks):
        load(chunk_at(step)).start()

    pointings = table_ref.shape[2]
    hot = (
        lax.broadcasted_iota(jnp.int32, (pointings, 2 * LANES), 0) == pick_ref[...]
    ).astype(bf16)

    def choose(s, carry):
        picked = jnp.dot(table_ref[s], hot, preferred_element_type=f32).astype(bf16)
        chosen[0, s] = picked[:, :LANES]
        chosen[1, s] = picked[:, LANES:]
        return carry

    lax.fori_loop(0, slots_here, choose, 0)

    def send_weights():
        pltpu.make_async_remote_copy(
            src_ref=chosen.at[other, mine],
            dst_ref=far_chosen.at[rank, mine],
            send_sem=w_send,
            recv_sem=w_recv.at[rank],
            device_id=(gate, tm),
            device_id_type=MESH,
        ).start()

    send_weights()
    lax.fori_loop(1, chunks, send_later, 0)

    def prepare_own(s, carry):
        prepare(chosen[side, s], own_w, s)
        return carry

    lax.fori_loop(0, slots_here, prepare_own, 0)

    tap_count = taps_ref.shape[0]
    repeat = lax.broadcasted_iota(jnp.int32, (chan, LANES), 0) == lax.rem(
        lax.broadcasted_iota(jnp.int32, (chan, LANES), 1), chan
    )
    taps = jnp.dot(
        taps_ref[...],
        repeat.astype(f32),
        precision=lax.Precision.HIGHEST,
        preferred_element_type=f32,
    )
    tap_at = lax.broadcasted_iota(jnp.int32, (tap_count, LANES), 0)
    time_at = lax.div(lax.broadcasted_iota(jnp.int32, (tap_count, LANES), 1), chan)
    for v in range(spans):
        row = jnp.sum(
            jnp.where(time_at - tap_at == v - halo, taps, 0.0), axis=0, keepdims=True
        )
        mat[v * 2 * chan : (v + 1) * 2 * chan] = (
            jnp.concatenate([row, row], axis=1) * trig_ref[...]
        ).astype(bf16)
    select_row = lax.broadcasted_iota(jnp.int32, (LANES, LANES), 0)
    phases = LANES // (2 * chan)
    select_time = lax.rem(select_row, LANES // phases) * phases + lax.div(
        select_row, LANES // phases
    )
    select[...] = (
        lax.broadcasted_iota(jnp.int32, (LANES, LANES), 1) == select_time
    ).astype(bf16)
    tail[...] = jnp.zeros_like(tail)

    def foreign_weights(k):
        forward = pltpu.make_async_remote_copy(
            src_ref=far_chosen.at[k, mine],
            dst_ref=far_chosen.at[k, mine],
            send_sem=fwd_send.at[k],
            recv_sem=fwd_recv.at[k],
            device_id=(me, 1 - tm),
            device_id_type=MESH,
        )
        drain(far_chosen.at[k, mine], w_recv.at[k])
        forward.start()
        drain(far_chosen.at[k, theirs], fwd_recv.at[k])

        def one(s, carry):
            prepare(far_chosen[k, s], far_w.at[k], s)
            return carry

        lax.fori_loop(0, slots_here, one, 0)
        drain(far_chosen.at[k, mine], fwd_send.at[k])

    def foreign(k, i, turn):
        c = chunk_at(i)
        slot = lax.rem(turn, ring)

        @pl.when(i == 0)
        def _():
            foreign_weights(k)

        @pl.when(turn >= ring)
        def _():
            wait_all(far_out.at[slot], far_sem.at[slot])

        src = source_of(k)

        def one(part, carry):
            first = part * batch
            drain(far_volts.at[c, k, pl.ds(first, batch)], volt_recv.at[c, k, part])
            form(far_w.at[k], far_volts.at[c, k], far_out.at[slot], src, c, first, batch)
            send_all(far_out.at[slot], src, c, far_sem.at[slot], first, batch)
            return carry

        lax.fori_loop(0, parts, one, 0)
        keep(far_out.at[slot], src, c)

    width = 2 * chan
    fold = LANES // width
    lanes_at = lax.broadcasted_iota(jnp.int32, (LANES // fold, LANES), 1)

    def swap(one, two, size):
        low = lax.rem(lanes_at, 2 * size) < size
        return (
            jnp.where(low, one, pltpu.roll(two, size, 1)),
            jnp.where(low, pltpu.roll(one, LANES - size, 1), two),
        )

    def exchange(parts):
        first, third = swap(parts[0], parts[2], 2 * width)
        second, fourth = swap(parts[1], parts[3], 2 * width)
        return swap(first, second, width) + swap(third, fourth, width)

    def synthesise(i):
        c = chunk_at(i - 1)

        def one(src, carry):
            local = (src == me) | (
                is_gate & (lax.div(src, half) == other) & (lax.rem(src, quarter) == lane)
            )

            @pl.when(jnp.logical_not(local))
            def _():
                drain(z.at[c, pl.ds(src * slots_here, slots_here)], z_sem.at[c, src])

            return carry

        lax.fori_loop(0, n, one, 0)

        def copy(s, carry):
            stage[s] = z[c, s]
            return carry

        lax.fori_loop(0, stage.shape[0], copy, 0, unroll=4)

        def gather(g, at_once):
            for k in range(chan):
                alive = g * chan + k < live_ref[0]
                block = stage[order_ref[g * chan + k]].astype(f32)
                wide[at_once, k * pitch : k * pitch + pair] = jnp.where(alive, block, 0.0)

            for q in range(group // fold):
                rows = [
                    wide[at_once, pl.ds(p * group + q * fold + b, chan, stride=pitch), :]
                    for b in range(fold)
                    for p in range(2)
                ]
                turned = lax.dot_general(
                    select[...],
                    jnp.concatenate(rows, axis=0).astype(bf16),
                    (((1,), (1,)), ((), ())),
                    preferred_element_type=f32,
                )
                size = LANES // fold
                split = [turned[w * size : (w + 1) * size] for w in range(fold)]
                for b, block in enumerate(exchange(split)):
                    beam = q * fold + b
                    at = g * group + beam
                    steps[at_once, beam, :8] = tail[at]
                    steps[at_once, beam, 8:] = block
                    tail[at] = block[LANES // fold - 8 :]
                    head[lax.min(i - 1, 1), at] = block[:8]
                    for e in range(spans // fold):
                        lhs[e, beam, pl.ds(pl.multiple_of(g * blocks, blocks), blocks)] = steps[
                            at_once, beam, pl.ds(8 - halo // fold + e, blocks, stride=inner // fold), :
                        ].astype(bf16)

        def several(j, carry):
            for at_once in range(together):
                gather(j * together + at_once, at_once)
            return carry

        lax.fori_loop(0, bands // together, several, 0)

        out_copy = pltpu.make_async_copy(
            ready,
            out_ref.at[:, :, pl.ds(pl.multiple_of(c * 2 * blocks, 2 * blocks), 2 * blocks)],
            out_sem,
        )

        @pl.when(i > 1)
        def _():
            drain(ready, out_sem)

        def emit(b, carry):
            rows = bands * blocks
            terms = [
                lhs[e, pl.ds(b * fold, fold)].reshape(fold * rows, LANES)
                for e in range(spans // fold)
            ]
            out = jnp.dot(
                jnp.concatenate(terms, axis=1), mat[...], preferred_element_type=f32
            )
            made[pl.ds(0, fold * rows, stride=2), :] = out[:, :LANES]
            made[pl.ds(1, fold * rows, stride=2), :] = out[:, LANES:]
            for j in range(fold):
                for g in range(bands):
                    at = (j * bands + g) * 2 * blocks
                    ready[b * fold + j, g] = made[at : at + 2 * blocks].astype(bf16)
            return carry

        lax.fori_loop(0, group // fold, emit, 0)
        out_copy.start()

    def patch():
        rows = halo // inner + 2
        opening = bands * rows

        def restack(b, carry):
            for g in range(bands):
                at = g * group + b
                joint[g, :8] = tail[at]
                joint[g, 8:] = head[0, at]
                for e in range(spans // fold):
                    redo[e, b, g * rows : (g + 1) * rows] = joint[
                        g, pl.ds(8 - halo // fold + e, rows, stride=inner // fold), :
                    ]
            return carry

        lax.fori_loop(0, group, restack, 0)
        terms = [
            redo[e].reshape(group * opening, LANES).astype(bf16) for e in range(spans // fold)
        ]
        out = jnp.dot(jnp.concatenate(terms, axis=1), mat[...], preferred_element_type=f32)
        made[pl.ds(0, group * opening, stride=2), :] = out[:, :LANES]
        made[pl.ds(1, group * opening, stride=2), :] = out[:, LANES:]

        def place(b, carry):
            for g in range(bands):
                at = pl.multiple_of(b * opening * 2 + g * rows * 2, rows * 2)
                mended[b, g] = made[pl.ds(at, rows * 2)].astype(bf16)
            return carry

        lax.fori_loop(0, group, place, 0)
        c = chunk_at(0)
        start = pl.multiple_of(c * 2 * blocks, 2 * blocks)
        copy = pltpu.make_async_copy(
            mended, out_ref.at[:, :, pl.ds(start, rows * 2)], mend_sem
        )
        copy.start()
        copy.wait()

    def pass_tail():
        return pltpu.make_async_remote_copy(
            src_ref=tail_sent,
            dst_ref=rim,
            send_sem=rim_sem.at[0],
            recv_sem=rim_sem.at[1],
            device_id=(me, 1),
            device_id_type=MESH,
        )

    def own(i, carry):
        c = chunk_at(i)
        form(own_w, volts.at[c], own_out.at[c], me, c, 0, slots_here)
        send_all(own_out.at[c], me, c, own_sem.at[c], 0, slots_here)
        keep(own_out.at[c], me, c)
        return carry

    ahead, prompt = 3, chunks
    lax.fori_loop(0, ahead, own, 0)

    def early(i, carry):
        later = i + ahead

        @pl.when((later < prompt) | (jnp.logical_not(is_gate) & (later < chunks)))
        def _():
            own(later, 0)

        @pl.when(is_gate)
        def _():
            foreign(1 - near, i, i)

        return carry

    lax.fori_loop(0, chunks, early, 0)

    def step(i, carry):
        @pl.when(is_gate & (i < chunks))
        def _():
            foreign(near, i, chunks + i)

        @pl.when(is_gate & (i + prompt < chunks))
        def _():
            own(i + prompt, 0)

        @pl.when((i == 2) & (tm == 0))
        def _():
            tail[...] = jnp.zeros_like(tail)

        @pl.when((i == 2) & (tm == 1))
        def _():
            drain(rim, rim_sem.at[1])

            def one(j, carry):
                tail[2 * j] = rim[j, :8].astype(f32)
                tail[2 * j + 1] = rim[j, 8:].astype(f32)
                return carry

            lax.fori_loop(0, rim.shape[0], one, 0)

        @pl.when(i >= 1)
        def _():
            synthesise(i)

        @pl.when((i == 1) & (tm == 0))
        def _():
            def one(j, carry):
                pair_at = jnp.concatenate([tail[2 * j], tail[2 * j + 1]], axis=0)
                tail_sent[j] = pair_at.astype(bf16)
                return carry

            lax.fori_loop(0, rim.shape[0], one, 0)
            pass_tail().start()

        return carry

    lax.fori_loop(0, chunks + 1, step, 0)
    patch()

    drain(ready, out_sem)
    drain(chosen.at[other, mine], w_send)

    @pl.when(tm == 0)
    def _():
        drain(tail_sent, rim_sem.at[0])

    def finish(c, carry):
        drain(volts.at[c], volt_send.at[c])
        wait_all(own_out.at[c], own_sem.at[c])
        return carry

    lax.fori_loop(0, chunks, finish, 0)

    @pl.when(is_gate)
    def _():
        def one(slot, carry):
            wait_all(far_out.at[slot], far_sem.at[slot])
            return carry

        lax.fori_loop(0, ring, one, 0)


def hand_over_kernel(in_ref, out_ref, held, in_sem, out_sem):
    count = held.shape[0]
    reads = [pltpu.make_async_copy(in_ref.at[b], held.at[b], in_sem.at[b]) for b in range(count)]
    writes = [
        pltpu.make_async_copy(held.at[b], out_ref.at[b], out_sem.at[b]) for b in range(count)
    ]
    for read in reads:
        read.start()
    for read, write in zip(reads, writes):
        read.wait()
        write.start()
    for write in writes:
        write.wait()


def pair_of(chan):
    return 2 * chan


def relay_plan(voltages, pointing_table, beam_pointing, subband_order, live_subbands, filter_taps):
    local, _, inputs, local_time = voltages.shape
    pointings = pointing_table.shape[2]
    beams = beam_pointing.shape[0]
    slots = subband_order.shape[0]
    tap_count, chan = filter_taps.shape
    n = lax.axis_size("sub")
    half = n // 2
    group = beams // n
    pair = 2 * group
    inner = LANES // chan
    spans = inner * (1 + -(-(tap_count - 1) // inner))
    halo = spans - inner
    chunks = local_time // LANES
    bands = slots // chan
    blocks = LANES // inner
    fold = LANES // (2 * chan)
    bf16, f32 = jnp.bfloat16, jnp.float32
    ring = 4
    together = math.gcd(bands, 4)

    at = np.arange(chan)
    phase = (np.outer(at, at) % chan).astype(np.float32) * np.float32(2.0 * math.pi / chan)
    cosine, sine = (
        np.asarray(f(phase), jnp.bfloat16).astype(np.float32) for f in (np.cos, np.sin)
    )
    trig = np.stack([np.stack([cosine, -sine], 1), np.stack([sine, cosine], 1)])
    trig = trig.transpose(2, 3, 0, 1)[:, :, :, None, :]
    trig = np.broadcast_to(trig, (2, chan, 2, inner, chan))
    trig = jnp.asarray(trig.reshape(2 * chan, 2 * LANES))
    signal = voltages.reshape(local, 2 * inputs, local_time)
    table = pointing_table.transpose(0, 1, 3, 2).reshape(local, 2 * inputs, pointings)
    lanes_in = 2 * LANES

    vmem = pl.BlockSpec(memory_space=pltpu.VMEM)
    smem = pl.BlockSpec(memory_space=pltpu.SMEM)
    anywhere = pl.BlockSpec(memory_space=pl.ANY)
    dma = pltpu.SemaphoreType.DMA
    out = pl.pallas_call(
        functools.partial(relay_kernel, n, chan),
        in_specs=[smem, smem, vmem, vmem, vmem, vmem, anywhere],
        out_specs=anywhere,
        out_shape=jax.ShapeDtypeStruct((group, bands, 2 * blocks * chunks, LANES), bf16),
        scratch_shapes=[
            pltpu.VMEM((chunks, slots, pair, LANES), bf16),
            pltpu.VMEM((chunks, half, local, pair, LANES), bf16),
            pltpu.VMEM((ring, half, local, pair, LANES), bf16),
            pltpu.VMEM((chunks, local, 2 * inputs, LANES), bf16),
            pltpu.VMEM((chunks, 2, local, 2 * inputs, LANES), bf16),
            pltpu.VMEM((2, local, 2 * inputs, LANES), bf16),
            pltpu.VMEM((2, local, 2 * inputs, LANES), bf16),
            pltpu.VMEM((local, half * pair, lanes_in), bf16),
            pltpu.VMEM((2, local, half * pair, lanes_in), bf16),
            pltpu.VMEM((spans // fold, group, bands * blocks, LANES), bf16),
            pltpu.VMEM((slots, pair, LANES), bf16),
            pltpu.VMEM((together, chan * (pair + 1), LANES), f32),
            pltpu.VMEM((LANES, LANES), bf16),
            pltpu.VMEM((together, group, 8 + LANES // fold, LANES), f32),
            pltpu.VMEM((spans * 2 * chan, 2 * LANES), bf16),
            pltpu.VMEM((fold * bands * blocks * 2, LANES), f32),
            pltpu.VMEM((group, bands, 2 * blocks, LANES), bf16),
            pltpu.VMEM((bands * group, 8, LANES), f32),
            pltpu.VMEM((bands * group // 2, 16, LANES), bf16),
            pltpu.VMEM((bands * group // 2, 16, LANES), bf16),
            pltpu.VMEM((2, bands * group, 8, LANES), f32),
            pltpu.VMEM((bands, 16, LANES), f32),
            pltpu.VMEM((spans // fold, group, bands * (halo // inner + 2), LANES), f32),
            pltpu.VMEM((group, bands, 2 * (halo // inner + 2), LANES), bf16),
            dma((chunks, n)),
            dma((chunks, half)),
            dma((ring, half)),
            dma((chunks,)),
            dma((chunks,)),
            dma((chunks, 2, 2)),
            dma,
            dma((2,)),
            dma((2,)),
            dma((2,)),
            dma((2,)),
            dma,
            dma,
        ],
        compiler_params=pltpu.CompilerParams(
            vmem_limit_bytes=66_000_000, has_side_effects=True
        ),
        cost_estimate=pl.CostEstimate(
            flops=20_000_000_000, bytes_accessed=20_000_000, transcendentals=0
        ),
        name="relay",
    )(
        subband_order,
        live_subbands,
        beam_pointing.reshape(1, beams),
        table,
        filter_taps,
        trig,
        signal,
    )
    out = pl.pallas_call(
        hand_over_kernel,
        in_specs=[anywhere],
        out_specs=anywhere,
        out_shape=jax.ShapeDtypeStruct(out.shape, bf16),
        scratch_shapes=[pltpu.VMEM(out.shape, bf16), dma((group,)), dma((group,))],
        compiler_params=pltpu.CompilerParams(vmem_limit_bytes=VMEM),
        name="hand_over",
    )(out)
    out = out.reshape(group, bands, blocks * chunks, 2, LANES).transpose(0, 1, 3, 2, 4)
    return out.reshape(group, bands, 2, local_time * chan)


def on_device(voltages, pointing_table, beam_pointing, subband_order, live_subbands, filter_taps):
    local, _, inputs, local_time = voltages.shape
    beams = beam_pointing.shape[0]
    tap_count, chan = filter_taps.shape
    n = lax.axis_size("sub")
    fits = (
        lax.axis_size("tm") == 2
        and n % 4 == 0
        and beams == 2 * LANES
        and beams // n % 8 == 0
        and local % 2 == 0
        and local_time % LANES == 0
        and local_time >= 4 * LANES
        and chan * 8 == LANES
        and tap_count <= chan + 1
    )
    plan = relay_plan if fits else direct_plan
    return plan(
        voltages, pointing_table, beam_pointing, subband_order, live_subbands, filter_taps
    )


def solution(mesh):
    in_specs = (P("sub", None, None, "tm"), P("sub", None, None, None), P(), P(), P(), P())
    out_specs = P("sub", None, None, "tm")
    return jax.shard_map(
        on_device, mesh=mesh, in_specs=in_specs, out_specs=out_specs, check_vma=False
    )
```
